8 devices in a mesh: dp: 2 (over z, y), cp: 4 (over x, core).
Axes of the slice: x: 2, y: 2, z: 1, core: 2. Of those that a mesh axis runs over, the one named last changes fastest.
Arguments:
- hidden: bfloat16 [32, 1024, 640], P('dp', 'cp'), parts along dimension 0
- positions: int32 [32, 1024], P('dp', 'cp'), parts along dimension 0
- wq_local: bfloat16 [640, 1024], replicated
- wk_local: bfloat16 [640, 256], replicated
- wv_local: bfloat16 [640, 256], replicated
- wo_local: bfloat16 [1024, 640], replicated
- wgate_local: bfloat16 [640, 2048], replicated
- wup_local: bfloat16 [640, 2048], replicated
- wdown_local: bfloat16 [2048, 640], replicated
- preatt_local: float32 [640], replicated
- postatt_local: float32 [640], replicated
- preffw_local: float32 [640], replicated
- postffw_local: float32 [640], replicated
- wq_global: bfloat16 [640, 1024], replicated
- wk_global: bfloat16 [640, 256], replicated
- wv_global: bfloat16 [640, 256], replicated
- wo_global: bfloat16 [1024, 640], replicated
- wgate_global: bfloat16 [640, 2048], replicated
- wup_global: bfloat16 [640, 2048], replicated
- wdown_global: bfloat16 [2048, 640], replicated
- preatt_global: float32 [640], replicated
- postatt_global: float32 [640], replicated
- preffw_global: float32 [640], replicated
- postffw_global: float32 [640], replicated
Outputs:
- output: bfloat16 [32, 1024, 640], P('dp', 'cp'), parts along dimension 0
There are 2 independent parts. The reference program is written for one: setup_inputs(seed, part) draws one part's arguments, and reference() takes and returns one part's arrays. A program takes and returns all parts, laid end to end along the dimension named above; an argument that names none is the same for every part.
All inputs are finite; a program needn't handle non-finite values.
Results may differ from the reference program's by a relative error of at most 0.02.
Values are sent between devices in bfloat16 or wider.
A program may use at most 1 GiB of HBM per device.

```python
import jax
import jax.numpy as jnp
from jax import lax

BATCH_ROWS = 16
SEQ_LEN = 1024
BLOCK_LEN = 256
MODEL_DIM = 640
NUM_HEADS = 4
KV_HEADS = 1
HEAD_DIM = 256
FFN_DIM = 2048
WINDOW = 512
NUM_BLOCKS = SEQ_LEN // BLOCK_LEN
GROUP_SIZE = NUM_HEADS // KV_HEADS
EPSILON = 1e-6
THETA = 10000.0
SOFT_CAP = 50.0
LAYER_TAGS = ("local", "global")
WEIGHT_NAMES = ("wq", "wk", "wv", "wo", "wgate", "wup", "wdown")
SCALE_NAMES = ("preatt", "postatt", "preffw", "postffw")


def layer_weights(rng_key, layer_tag):
    key_list = jax.random.split(rng_key, 11)
    q_width = NUM_HEADS * HEAD_DIM
    kv_width = KV_HEADS * HEAD_DIM
    shapes = ((MODEL_DIM, q_width), (MODEL_DIM, kv_width), (MODEL_DIM, kv_width), (q_width, MODEL_DIM), (MODEL_DIM, FFN_DIM), (MODEL_DIM, FFN_DIM), (FFN_DIM, MODEL_DIM))
    weights = {}
    for slot_idx in range(7):
        fan_in, fan_out = shapes[slot_idx]
        drawn = jax.random.normal(key_list[slot_idx], (fan_in, fan_out), jnp.float32) * fan_in ** -0.5
        weights[WEIGHT_NAMES[slot_idx] + "_" + layer_tag] = drawn.astype(jnp.bfloat16)
    for slot_idx in range(4):
        weights[SCALE_NAMES[slot_idx] + "_" + layer_tag] = 0.4 * jax.random.normal(key_list[7 + slot_idx], (MODEL_DIM,), jnp.float32)
    return weights


def setup_inputs(seed: int = 0, part: int = 0) -> dict:
    part_key = jax.random.fold_in(jax.random.key(seed), part)
    key_hidden, key_steps = jax.random.split(part_key)
    hidden = jax.random.normal(key_hidden, (BATCH_ROWS, SEQ_LEN, MODEL_DIM), jnp.float32).astype(jnp.bfloat16)
    step_sizes = jax.random.randint(key_steps, (BATCH_ROWS, SEQ_LEN), 1, 3, jnp.int32)
    positions = (jnp.cumsum(step_sizes, axis=1) - step_sizes[:, :1]).astype(jnp.int32)
    inputs = {"hidden": hidden, "positions": positions}
    weight_key = jax.random.key(seed + 1)
    for layer_idx in range(2):
        inputs.update(layer_weights(jax.random.fold_in(weight_key, layer_idx), LAYER_TAGS[layer_idx]))
    return inputs


def rms_norm(inputs, norm_scale):
    widened = inputs.astype(jnp.float32)
    mean_sq = jnp.mean(widened * widened, axis=-1, keepdims=True)
    return (widened * lax.rsqrt(mean_sq + EPSILON) * (1.0 + norm_scale)).astype(jnp.bfloat16)


def mat_mul(inputs, weight):
    flat_in = inputs.reshape(-1, inputs.shape[-1])
    product = jnp.dot(flat_in, weight, preferred_element_type=jnp.float32)
    return product.reshape(inputs.shape[:-1] + (weight.shape[1],)).astype(jnp.bfloat16)


def apply_rope(heads_in, positions):
    half_dim = HEAD_DIM // 2
    inv_freq = THETA ** (-(jnp.arange(half_dim, dtype=jnp.float32) * 2.0 / HEAD_DIM))
    angles = positions.astype(jnp.float32)[:, :, None, None] * inv_freq
    cos_t = jnp.cos(angles)
    sin_t = jnp.sin(angles)
    widened = heads_in.astype(jnp.float32)
    first_half = widened[..., :half_dim]
    second_half = widened[..., half_dim:]
    return jnp.concatenate([first_half * cos_t - second_half * sin_t, second_half * cos_t + first_half * sin_t], axis=-1)


def decoder_layer(hidden, positions, weights, window_len):
    w_q, w_k, w_v, w_o, w_gate, w_up, w_down, pre_att, post_att, pre_ffw, post_ffw = weights
    normed = rms_norm(hidden, pre_att)
    query_rot = apply_rope(mat_mul(normed, w_q).reshape(BATCH_ROWS, SEQ_LEN, NUM_HEADS, HEAD_DIM), positions)
    query_rot = (query_rot * HEAD_DIM ** -0.5).astype(jnp.bfloat16)
    key_rot = apply_rope(mat_mul(normed, w_k).reshape(BATCH_ROWS, SEQ_LEN, KV_HEADS, HEAD_DIM), positions).astype(jnp.bfloat16)
    value_t = mat_mul(normed, w_v).reshape(BATCH_ROWS, SEQ_LEN, KV_HEADS, HEAD_DIM)
    key_wide = key_rot.astype(jnp.float32)
    value_wide = value_t.astype(jnp.float32)
    q_blocks = query_rot.reshape(BATCH_ROWS, NUM_BLOCKS, BLOCK_LEN, KV_HEADS, GROUP_SIZE, HEAD_DIM).transpose(1, 0, 2, 3, 4, 5)
    pos_blocks = positions.reshape(BATCH_ROWS, NUM_BLOCKS, BLOCK_LEN).transpose(1, 0, 2)
    hid_blocks = hidden.reshape(BATCH_ROWS, NUM_BLOCKS, BLOCK_LEN, MODEL_DIM).transpose(1, 0, 2, 3)

    def one_block(block_in):
        q_block, q_pos, h_block = block_in
        scores = jnp.einsum("bqkgd,bskd->bkgqs", q_block.astype(jnp.float32), key_wide)
        capped = SOFT_CAP * jnp.tanh(scores / SOFT_CAP)
        offset = q_pos[:, None, None, :, None] - positions[:, None, None, None, :]
        visible = (offset >= 0) & (offset < window_len)
        prob_bf = jax.nn.softmax(jnp.where(visible, capped, -1e30), axis=-1).astype(jnp.bfloat16)
        mixed_heads = jnp.einsum("bkgqs,bskd->bqkgd", prob_bf.astype(jnp.float32), value_wide).astype(jnp.bfloat16)
        attn_out = mat_mul(mixed_heads.reshape(BATCH_ROWS, BLOCK_LEN, NUM_HEADS * HEAD_DIM), w_o)
        mid_state = (h_block.astype(jnp.float32) + rms_norm(attn_out, post_att).astype(jnp.float32)).astype(jnp.bfloat16)
        normed_mid = rms_norm(mid_state, pre_ffw)
        gate_val = mat_mul(normed_mid, w_gate)
        up_val = mat_mul(normed_mid, w_up)
        act_val = (jax.nn.gelu(gate_val.astype(jnp.float32), approximate=True) * up_val.astype(jnp.float32)).astype(jnp.bfloat16)
        down_val = mat_mul(act_val, w_down)
        return (mid_state.astype(jnp.float32) + rms_norm(down_val, post_ffw).astype(jnp.float32)).astype(jnp.bfloat16)

    out_blocks = lax.map(one_block, (q_blocks, pos_blocks, hid_blocks))
    return out_blocks.transpose(1, 0, 2, 3).reshape(BATCH_ROWS, SEQ_LEN, MODEL_DIM)


def reference(hidden, positions, wq_local, wk_local, wv_local, wo_local, wgate_local, wup_local, wdown_local, preatt_local, postatt_local, preffw_local, postffw_local, wq_global, wk_global, wv_global, wo_global, wgate_global, wup_global, wdown_global, preatt_global, postatt_global, preffw_global, postffw_global):
    local_set = (wq_local, wk_local, wv_local, wo_local, wgate_local, wup_local, wdown_local, preatt_local, postatt_local, preffw_local, postffw_local)
    global_set = (wq_global, wk_global, wv_global, wo_global, wgate_global, wup_global, wdown_global, preatt_global, postatt_global, preffw_global, postffw_global)
    mid_hidden = decoder_layer(hidden, positions, local_set, WINDOW)
    return decoder_layer(mid_hidden, positions, global_set, 2 * SEQ_LEN)
```

```python
import functools

import jax
import jax.numpy as jnp
import numpy as np
from jax import lax
from jax.experimental import pallas as pl
from jax.experimental.pallas import tpu as pltpu
from jax.sharding import PartitionSpec as P

DIM = 640
HEADS = 4
HD = 256
HALF = HD // 2
FFN = 2048
WINDOW = 512
EPSILON = 1e-6
THETA = 10000.0
SOFT_CAP = 50.0
LOG2E = 1.4426950408889634
BLK = 256
NCP = 4
ROWS = 4
QKV = HEADS * HD + 2 * HD
FCH = 512
LOW = 64
HIGH = 32
BF = jnp.bfloat16
F32 = jnp.float32


def rope_lookup():
    inv_freq = THETA ** (-(np.arange(HALF, dtype=np.float64) * 2.0 / HD))
    table = np.zeros((128, 4 * HALF), np.float64)
    high = np.arange(HIGH)[:, None] * float(LOW) * inv_freq
    low = np.arange(LOW)[:, None] * inv_freq
    table[:HIGH, 0:HALF] = np.cos(high)
    table[:HIGH, HALF : 2 * HALF] = np.sin(high)
    table[HIGH : HIGH + LOW, 2 * HALF : 3 * HALF] = np.cos(low)
    table[HIGH : HIGH + LOW, 3 * HALF :] = np.sin(low)
    parts = []
    rest = table
    for _ in range(3):
        part = rest.astype(jnp.bfloat16)
        parts.append(part)
        rest = rest - part.astype(np.float64)
    return np.concatenate(parts, axis=1)


def dot(lhs, rhs):
    return jnp.dot(lhs, rhs, preferred_element_type=F32)


def rms(wide, gain):
    mean_sq = jnp.mean(wide * wide, axis=-1, keepdims=True)
    return (wide * lax.rsqrt(mean_sq + EPSILON) * gain).astype(BF)


def kernel(
    hid, pos, gains, table, *rest
):
    weights = rest[:14]
    out = rest[14]
    (x_buf, pos_buf, w_qkv, w_o, w_gu, w_d, k_buf, v_buf, q_buf, o_buf, e_buf, h_buf, cos_buf, sin_buf, qp_buf,
     w_sem, in_send, in_recv, pos_send, pos_recv, out_send, out_recv) = rest[15:]
    me = lax.axis_index("cp")

    def weight_copies(layer):
        w_q, w_k, w_v, wo, wg, wu, wd = weights[7 * layer : 7 * layer + 7]
        places = (
            (w_q, w_qkv.at[layer, :, 0:1024]),
            (w_k, w_qkv.at[layer, :, 1024:1280]),
            (w_v, w_qkv.at[layer, :, 1280:1536]),
            (wo, w_o.at[layer]),
            (wg, w_gu.at[layer, :, 0:FFN]),
            (wu, w_gu.at[layer, :, FFN : 2 * FFN]),
            (wd, w_d.at[layer]),
        )
        return [pltpu.make_async_copy(src, dst, w_sem.at[layer, i]) for i, (src, dst) in enumerate(places)]

    def peer(shift):
        return lax.rem(me + shift, NCP)

    def send_piece(row, dest):
        return pltpu.make_async_remote_copy(
            src_ref=hid.at[dest * ROWS + row],
            dst_ref=x_buf.at[row, me],
            send_sem=in_send.at[row, dest],
            recv_sem=in_recv.at[row, me],
            device_id={"cp": dest},
            device_id_type=pl.DeviceIdType.MESH,
        )

    def own_piece(row):
        return pltpu.make_async_copy(hid.at[me * ROWS + row], x_buf.at[row, me], in_recv.at[row, me])

    def send_pos(dest):
        return pltpu.make_async_remote_copy(
            src_ref=pos.at[dest],
            dst_ref=pos_buf.at[me],
            send_sem=pos_send.at[dest],
            recv_sem=pos_recv.at[me],
            device_id={"cp": dest},
            device_id_type=pl.DeviceIdType.MESH,
        )

    def own_pos():
        return pltpu.make_async_copy(pos.at[me], pos_buf.at[me], pos_recv.at[me])

    def send_out(row, piece):
        return pltpu.make_async_remote_copy(
            src_ref=x_buf.at[row, piece],
            dst_ref=out.at[me * ROWS + row],
            send_sem=out_send.at[row, piece],
            recv_sem=out_recv.at[me * ROWS + row],
            device_id={"cp": piece},
            device_id_type=pl.DeviceIdType.MESH,
        )

    def own_out(row):
        return pltpu.make_async_copy(x_buf.at[row, me], out.at[me * ROWS + row], out_send.at[row, me])

    for copy in weight_copies(0)[:3]:
        copy.start()
    own_piece(0).start()
    own_pos().start()

    barrier = pltpu.get_barrier_semaphore()
    for shift in range(1, NCP):
        pl.semaphore_signal(barrier, inc=1, device_id={"cp": peer(shift)}, device_id_type=pl.DeviceIdType.MESH)
    pl.semaphore_wait(barrier, NCP - 1)

    core = lax.rem(me, 2)
    partner = me + 1 - 2 * core
    far_0 = lax.rem(me + 2 - core, NCP)
    far_1 = lax.rem(me + 3 - core, NCP)
    for shift in range(1, NCP):
        send_pos(peer(shift)).start()
    send_piece(0, partner).start()

    @pl.when(core == 0)
    def _():
        send_piece(0, far_0).start()
        send_piece(0, far_1).start()

    for copy in weight_copies(0)[3:] + weight_copies(1):
        copy.start()
    for row in range(1, ROWS):
        own_piece(row).start()
    own_pos().wait()
    for shift in range(1, NCP):
        src = peer(shift)
        pltpu.make_async_copy(pos_buf.at[src], pos_buf.at[src], pos_recv.at[src]).wait()

    def attention(layer, first, count, row):
        keys = count * BLK
        base = pl.multiple_of(first * BLK, BLK) if not isinstance(first, int) else first * BLK
        below = lax.broadcasted_iota(jnp.int32, (BLK, BLK), 0) >= lax.broadcasted_iota(jnp.int32, (BLK, BLK), 1)
        q_low = qp_buf[...] - float(WINDOW)
        for head in range(HEADS):
            query = q_buf[head]
            total = jnp.zeros((BLK, 128), F32)
            for j in range(count):
                key = k_buf[layer, pl.ds(base + j * BLK, BLK), :]
                score = lax.dot_general(query, key, (((1,), (1,)), ((), ())), preferred_element_type=F32)
                soft = jnp.exp2(jnp.tanh(score * (1.0 / SOFT_CAP)) * (SOFT_CAP * LOG2E))
                if j == count - 1:
                    soft = jnp.where(below, soft, 0.0)
                elif layer == 0:
                    k_pos = pos_buf[first + j, pl.ds(row, 1), :].astype(F32)
                    halves = []
                    for lo in (0, 128):
                        halves.append(jnp.where(q_low < k_pos[:, lo : lo + 128], soft[:, lo : lo + 128], 0.0))
                    soft = jnp.concatenate(halves, axis=1)
                e_buf[head, :, j * BLK : (j + 1) * BLK] = soft
                total = total + (soft[:, :128] + soft[:, 128:])
            inverse = 1.0 / jnp.sum(total, axis=-1, keepdims=True)
            prob = (e_buf[head, :, 0:keys] * inverse).astype(BF)
            mixed = dot(prob, v_buf[layer, pl.ds(base, keys), :])
            o_buf[:, head * HD : (head + 1) * HD] = mixed.astype(BF)

    def step(it, carry):
        layer = lax.rem(it, 2)
        piece = lax.rem(it // 2, NCP)
        row = it // (2 * NCP)
        x_ref = x_buf.at[row, piece]

        @pl.when(layer == 0)
        def _():
            pltpu.make_async_copy(x_ref, x_ref, in_recv.at[row, piece]).wait()
            row_pos = pos_buf[piece, pl.ds(row, 1), :]
            col_pos = jnp.transpose(jnp.broadcast_to(row_pos.astype(F32), (128, BLK)))
            qp_buf[...] = col_pos
            whole = col_pos.astype(jnp.int32)
            lane = lax.broadcasted_iota(jnp.int32, (BLK, 128), 1)
            hit = (lane == (whole >> 6)) | (lane == (whole & (LOW - 1)) + HIGH)
            found = dot(jnp.where(hit, 1.0, 0.0).astype(BF), table[...])
            width = 4 * HALF
            found = found[:, :width] + found[:, width : 2 * width] + found[:, 2 * width :]
            c_hi, s_hi = found[:, 0:HALF], found[:, HALF : 2 * HALF]
            c_lo, s_lo = found[:, 2 * HALF : 3 * HALF], found[:, 3 * HALF :]
            cos_buf[...] = c_hi * c_lo - s_hi * s_lo
            sin_buf[...] = s_hi * c_lo + c_hi * s_lo

        for first in range(2):
            @pl.when(it == first)
            def _():
                for copy in weight_copies(first)[:3]:
                    copy.wait()

        @pl.when((it == 1) & (core == 1))
        def _():
            send_piece(0, far_0).start()
            send_piece(0, far_1).start()

        @pl.when((piece == 1) & (layer == 0) & (row < ROWS - 1))
        def _():
            for dest in (partner, far_0, far_1):
                send_piece(row + 1, dest).start()

        normed = rms(x_ref[...].astype(F32), gains[pl.ds(layer * 4, 1), :])
        cos_t, sin_t = cos_buf[...], sin_buf[...]
        spot = pl.multiple_of(piece * BLK, BLK)

        def rotate(raw):
            wide = raw.astype(BF).astype(F32)
            one, two = wide[:, :HALF], wide[:, HALF:]
            return one * cos_t - two * sin_t, two * cos_t + one * sin_t

        for head in range(HEADS):
            one, two = rotate(dot(normed, w_qkv[layer, :, head * HD : (head + 1) * HD]))
            q_buf[head, :, :HALF] = (one * HD**-0.5).astype(BF)
            q_buf[head, :, HALF:] = (two * HD**-0.5).astype(BF)
        one, two = rotate(dot(normed, w_qkv[layer, :, 1024:1280]))
        k_buf[layer, pl.ds(spot, BLK), :HALF] = one.astype(BF)
        k_buf[layer, pl.ds(spot, BLK), HALF:] = two.astype(BF)
        v_buf[layer, pl.ds(spot, BLK), :] = dot(normed, w_qkv[layer, :, 1280:1536]).astype(BF)

        for count in range(1, 4):
            @pl.when((layer == 0) & (jnp.minimum(piece, 2) == count - 1))
            def _():
                attention(0, piece - (count - 1), count, row)
        for count in range(1, 5):
            @pl.when((layer == 1) & (piece == count - 1))
            def _():
                attention(1, 0, count, row)

        for first in range(2):
            @pl.when(it == first)
            def _():
                for copy in weight_copies(first)[3:]:
                    copy.wait()

        attn = dot(o_buf[...], w_o[layer]).astype(BF)
        delta = rms(attn.astype(F32), gains[pl.ds(layer * 4 + 1, 1), :])
        mid = (x_ref[...].astype(F32) + delta.astype(F32)).astype(BF)
        x_ref[...] = mid
        normed_mid = rms(mid.astype(F32), gains[pl.ds(layer * 4 + 2, 1), :])
        for lo in range(0, FFN, FCH):
            gate = dot(normed_mid, w_gu[layer, :, lo : lo + FCH]).astype(BF).astype(F32)
            up = dot(normed_mid, w_gu[layer, :, FFN + lo : FFN + lo + FCH]).astype(BF).astype(F32)
            inner = gate * (0.7978845608028654 + (0.7978845608028654 * 0.044715) * (gate * gate))
            h_buf[:, lo : lo + FCH] = ((0.5 * gate) * (1.0 + jnp.tanh(inner)) * up).astype(BF)
        down = dot(h_buf[...], w_d[layer]).astype(BF)
        delta = rms(down.astype(F32), gains[pl.ds(layer * 4 + 3, 1), :])
        x_ref[...] = (x_ref[...].astype(F32) + delta.astype(F32)).astype(BF)

        @pl.when((layer == 1) & (piece == me))
        def _():
            own_out(row).start()

        @pl.when((layer == 1) & (piece != me))
        def _():
            send_out(row, piece).start()

        return carry

    lax.fori_loop(0, ROWS * NCP * 2, step, 0)

    for shift in range(1, NCP):
        other = peer(shift)
        send_pos(other).wait_send()
        for row in range(ROWS):
            send_piece(row, other).wait_send()
            send_out(row, other).wait_send()
            place = out.at[other * ROWS + row]
            pltpu.make_async_copy(place, place, out_recv.at[other * ROWS + row]).wait()
    for row in range(ROWS):
        own_out(row).wait()


def device_step(hidden, positions, *params):
    local_w, global_w = params[:11], params[11:]
    gains = 1.0 + jnp.stack([*local_w[7:], *global_w[7:]])
    table = jnp.asarray(rope_lookup())
    pos = positions.reshape(NCP, ROWS, BLK)
    hbm = pl.BlockSpec(memory_space=pl.ANY)
    vmem = pl.BlockSpec(memory_space=pltpu.VMEM)
    dma = pltpu.SemaphoreType.DMA
    return pl.pallas_call(
        kernel,
        out_shape=jax.ShapeDtypeStruct(hidden.shape, hidden.dtype),
        in_specs=[hbm, hbm, vmem, vmem] + [hbm] * 14,
        out_specs=hbm,
        scratch_shapes=[
            pltpu.VMEM((ROWS, NCP, BLK, DIM), BF),
            pltpu.VMEM((NCP, ROWS, BLK), jnp.int32),
            pltpu.VMEM((2, DIM, QKV), BF),
            pltpu.VMEM((2, HEADS * HD, DIM), BF),
            pltpu.VMEM((2, DIM, 2 * FFN), BF),
            pltpu.VMEM((2, FFN, DIM), BF),
            pltpu.VMEM((2, NCP * BLK, HD), BF),
            pltpu.VMEM((2, NCP * BLK, HD), BF),
            pltpu.VMEM((HEADS, BLK, HD), BF),
            pltpu.VMEM((BLK, HEADS * HD), BF),
            pltpu.VMEM((HEADS, BLK, NCP * BLK), F32),
            pltpu.VMEM((BLK, FFN), BF),
            pltpu.VMEM((BLK, HALF), F32),
            pltpu.VMEM((BLK, HALF), F32),
            pltpu.VMEM((BLK, 128), F32),
            dma((2, 7)),
            dma((ROWS, NCP)),
            dma((ROWS, NCP)),
            dma((NCP,)),
            dma((NCP,)),
            dma((ROWS, NCP)),
            dma((NCP * ROWS,)),
        ],
        compiler_params=pltpu.CompilerParams(
            collective_id=0, has_side_effects=True, vmem_limit_bytes=60 * 1024 * 1024
        ),
        name="layers",
    )(hidden, pos, gains, table, *local_w[:7], *global_w[:7])


def solution(mesh):
    specs_in = tuple([P("dp", "cp"), P("dp", "cp")] + [P()] * 22)
    return jax.shard_map(device_step, mesh=mesh, in_specs=specs_in, out_specs=P("dp", "cp"), check_vma=False)
```

```python
import functools

import jax
import jax.numpy as jnp
import numpy as np
from jax import lax
from jax.experimental import pallas as pl
from jax.experimental.pallas import tpu as pltpu
from jax.sharding import PartitionSpec as P

DIM = 640
HEADS = 4
HD = 256
HALF = HD // 2
FFN = 2048
WINDOW = 512
EPSILON = 1e-6
THETA = 10000.0
SOFT_CAP = 50.0
LOG2E = 1.4426950408889634
BLK = 256
NCP = 4
ROWS = 4
UNITS = ROWS * NCP * 2
QKV = HEADS * HD + 2 * HD
FCH = 256
NROW = 64
NCH = {0: 256, 256: 256, 512: 128}
LOW = 64
HIGH = 32
BF = jnp.bfloat16
F32 = jnp.float32
MESH = pl.DeviceIdType.MESH


def rope_lookup():
    inv_freq = THETA ** (-(np.arange(HALF, dtype=np.float64) * 2.0 / HD))
    table = np.zeros((128, 4 * HALF), np.float64)
    high = np.arange(HIGH)[:, None] * float(LOW) * inv_freq
    low = np.arange(LOW)[:, None] * inv_freq
    table[:HIGH, 0:HALF] = np.cos(high)
    table[:HIGH, HALF : 2 * HALF] = np.sin(high)
    table[HIGH : HIGH + LOW, 2 * HALF : 3 * HALF] = np.cos(low)
    table[HIGH : HIGH + LOW, 3 * HALF :] = np.sin(low)
    parts = []
    rest = table
    for _ in range(3):
        part = rest.astype(jnp.bfloat16)
        parts.append(part)
        rest = rest - part.astype(np.float64)
    return np.concatenate(parts, axis=0)


def dot(lhs, rhs):
    return jnp.dot(lhs, rhs, preferred_element_type=F32)


def rms(wide, gain):
    mean_sq = jnp.mean(wide * wide, axis=-1, keepdims=True)
    tall = (wide * lax.rsqrt(mean_sq + EPSILON)).reshape(-1, 8, DIM) * gain[None]
    return tall.reshape(-1, DIM).astype(BF)


def unit(k):
    stream = lax.rem(k, 2)
    turn = k // 2
    layer = lax.rem(turn, 2)
    piece = lax.rem(turn // 2, NCP)
    row = (turn // (2 * NCP)) * 2 + stream
    return stream, layer, piece, row


def kernel(hid, pos, table, *rest):
    scales = rest[:8]
    weights = rest[8:22]
    out = rest[22]
    (x_buf, pos_buf, w_qkv, w_o, w_gu, w_d, k_buf, v_buf, q_buf, o_buf, e_buf, h_buf, a_buf, m_buf, t_buf, d_buf, mid_buf, cos_buf,
     sin_buf, qp_buf, gains, w_sem, in_send, in_recv, pos_send, pos_recv, out_send, out_recv) = rest[23:]
    me = lax.axis_index("cp")

    def weight_copies(layer):
        w_q, w_k, w_v, wo, wg, wu, wd = weights[7 * layer : 7 * layer + 7]
        places = (
            (w_q, w_qkv.at[layer, :, 0:1024]),
            (w_k, w_qkv.at[layer, :, 1024:1280]),
            (w_v, w_qkv.at[layer, :, 1280:1536]),
            (wo, w_o.at[layer]),
            (wg, w_gu.at[layer, :, 0:FFN]),
            (wu, w_gu.at[layer, :, FFN : 2 * FFN]),
            (wd, w_d.at[layer]),
        )
        return [pltpu.make_async_copy(src, dst, w_sem.at[layer, i]) for i, (src, dst) in enumerate(places)]

    def peer(shift):
        return lax.rem(me + shift, NCP)

    def send_piece(row, dest):
        return pltpu.make_async_remote_copy(
            src_ref=hid.at[dest * ROWS + row],
            dst_ref=x_buf.at[row * NCP + me],
            send_sem=in_send.at[row, dest],
            recv_sem=in_recv.at[row * NCP + me],
            device_id={"cp": dest},
            device_id_type=MESH,
        )

    def own_piece(row):
        return pltpu.make_async_copy(hid.at[me * ROWS + row], x_buf.at[row * NCP + me], in_recv.at[row * NCP + me])

    def send_pos(dest):
        return pltpu.make_async_remote_copy(
            src_ref=pos,
            dst_ref=pos_buf.at[me],
            send_sem=pos_send.at[dest],
            recv_sem=pos_recv.at[me],
            device_id={"cp": dest},
            device_id_type=MESH,
        )

    def own_pos():
        return pltpu.make_async_copy(pos, pos_buf.at[me], pos_recv.at[me])

    def send_out(row, piece):
        return pltpu.make_async_remote_copy(
            src_ref=x_buf.at[row * NCP + piece],
            dst_ref=out.at[me * ROWS + row],
            send_sem=out_send.at[row, piece],
            recv_sem=out_recv.at[me * ROWS + row],
            device_id={"cp": piece},
            device_id_type=MESH,
        )

    def own_out(row):
        return pltpu.make_async_copy(x_buf.at[row * NCP + me], out.at[me * ROWS + row], out_send.at[row, me])

    for copy in weight_copies(0)[:3]:
        copy.start()
    own_piece(0).start()
    own_pos().start()
    own_piece(1).start()

    barrier = pltpu.get_barrier_semaphore()
    for shift in range(1, NCP):
        pl.semaphore_signal(barrier, inc=1, device_id={"cp": peer(shift)}, device_id_type=MESH)
    pl.semaphore_wait(barrier, NCP - 1)

    core = lax.rem(me, 2)
    partner = me + 1 - 2 * core
    far_0 = lax.rem(me + 2 - core, NCP)
    far_1 = lax.rem(me + 3 - core, NCP)
    for shift in range(1, NCP):
        send_pos(peer(shift)).start()
    for row in range(2):
        send_piece(row, partner).start()

    @pl.when(core == 0)
    def _():
        for row in range(2):
            send_piece(row, far_0).start()
            send_piece(row, far_1).start()

    for copy in weight_copies(0)[3:] + weight_copies(1):
        copy.start()
    for row in range(2, ROWS):
        own_piece(row).start()
    for i in range(8):
        gains[i] = jnp.broadcast_to(1.0 + scales[i][...].reshape(1, DIM), (8, DIM))
    own_pos().wait()
    for shift in range(1, NCP):
        src = peer(shift)
        pltpu.make_async_copy(pos_buf.at[src], pos_buf.at[src], pos_recv.at[src]).wait()

    def positions_of(piece, row):
        return pos_buf[piece, pl.ds(me * ROWS + row, 1), :].astype(F32)

    def receive(k):
        _, _, piece, row = unit(k)
        x_ref = x_buf.at[row * NCP + piece]
        pltpu.make_async_copy(x_ref, x_ref, in_recv.at[row * NCP + piece]).wait()

    def rope(stream, index, half):
        piece = lax.rem(index, NCP)
        row = jnp.minimum(index // NCP, 1) * 2 + stream
        slot = stream * 2 + lax.rem(index, 2)
        spot = pl.multiple_of(half * 128, 128)
        whole_row = positions_of(piece, row)
        row_pos = jnp.where(half == 0, whole_row[:, :128], whole_row[:, 128:])
        col_pos = jnp.transpose(jnp.broadcast_to(row_pos, (128, 128)))
        whole = col_pos.astype(jnp.int32)
        lane = lax.broadcasted_iota(jnp.int32, (128, 128), 1)
        hit = jnp.where((lane == (whole >> 6)) | (lane == (whole & (LOW - 1)) + HIGH), 1.0, 0.0).astype(BF)
        found = dot(jnp.concatenate([hit, hit], axis=1), table[0:256, :]) + dot(hit, table[256:384, :])
        c_hi, s_hi = found[:, 0:HALF], found[:, HALF : 2 * HALF]
        c_lo, s_lo = found[:, 2 * HALF : 3 * HALF], found[:, 3 * HALF :]
        qp_buf[slot, pl.ds(spot, 128), :] = col_pos
        cos_buf[slot, pl.ds(spot, 128), :] = c_hi * c_lo - s_hi * s_lo
        sin_buf[slot, pl.ds(spot, 128), :] = s_hi * c_lo + c_hi * s_lo

    def enter(k):
        _, layer, piece, row = unit(k)
        for lo in range(0, BLK, NROW):
            part = x_buf[row * NCP + piece, lo : lo + NROW, :].astype(F32)
            a_buf[lo : lo + NROW, :] = rms(part, gains[layer * 4])

    def attend(k, count):
        stream, layer, piece, row = unit(k)
        turn = stream * 2 + lax.rem(piece, 2)
        cos_t, sin_t = cos_buf[turn], sin_buf[turn]
        spot = pl.multiple_of(piece * BLK, BLK)
        keys = count * BLK
        first = piece - (count - 1)
        base = pl.multiple_of(first * BLK, BLK)
        below = lax.broadcasted_iota(jnp.int32, (BLK, BLK), 0) >= lax.broadcasted_iota(jnp.int32, (BLK, BLK), 1)
        window = jnp.where(layer == 0, float(WINDOW), 65536.0)
        q_low = qp_buf[turn] - window
        totals = {}

        def rotate(raw):
            wide = raw.astype(BF).astype(F32)
            one, two = wide[:, :HALF], wide[:, HALF:]
            return one * cos_t - two * sin_t, two * cos_t + one * sin_t

        def key_value():
            normed = a_buf[...]
            one, two = rotate(dot(normed, w_qkv[layer, :, 1024:1280]))
            k_buf[stream, layer, pl.ds(spot, BLK), :HALF] = one.astype(BF)
            k_buf[stream, layer, pl.ds(spot, BLK), HALF:] = two.astype(BF)
            v_buf[stream, layer, pl.ds(spot, BLK), :] = dot(normed, w_qkv[layer, :, 1280:1536]).astype(BF)

        def query(head):
            one, two = rotate(dot(a_buf[...], w_qkv[layer, :, head * HD : (head + 1) * HD]))
            q_buf[head, :, :HALF] = (one * HD**-0.5).astype(BF)
            q_buf[head, :, HALF:] = (two * HD**-0.5).astype(BF)

        def score(head, j):
            key = k_buf[stream, layer, pl.ds(base + j * BLK, BLK), :]
            raw = lax.dot_general(q_buf[head], key, (((1,), (1,)), ((), ())), preferred_element_type=F32)
            soft = jnp.exp2(jnp.tanh(raw * (1.0 / SOFT_CAP)) * (SOFT_CAP * LOG2E))
            if j == count - 1:
                soft = jnp.where(below, soft, 0.0)
            elif count < NCP:
                k_pos = positions_of(first + j, row)
                halves = []
                for lo in (0, 128):
                    halves.append(jnp.where(q_low < k_pos[:, lo : lo + 128], soft[:, lo : lo + 128], 0.0))
                soft = jnp.concatenate(halves, axis=1)
            e_buf[head, :, j * BLK : (j + 1) * BLK] = soft
            part = soft[:, :128] + soft[:, 128:]
            totals[head] = part if j == 0 else totals[head] + part
            if j == count - 1:
                totals[head] = 1.0 / jnp.sum(totals[head], axis=-1, keepdims=True)

        def mix(head):
            prob = (e_buf[head, :, 0:keys] * totals[head]).astype(BF)
            mixed = dot(prob, v_buf[stream, layer, pl.ds(base, keys), :])
            o_buf[stream, :, head * HD : (head + 1) * HD] = mixed.astype(BF)

        return key_value, query, score, mix

    def finish(k):
        stream, layer, piece, row = unit(k)
        kept = {}

        def project(lo):
            t_buf[:, lo : lo + NCH[lo]] = dot(o_buf[stream], w_o[layer, :, lo : lo + NCH[lo]]).astype(BF)

        def norms():
            for lo in range(0, BLK, NROW):
                delta = rms(t_buf[lo : lo + NROW, :].astype(F32), gains[layer * 4 + 1])
                part = x_buf[row * NCP + piece, lo : lo + NROW, :].astype(F32)
                mid = (part + delta.astype(F32)).astype(BF)
                mid_buf[lo : lo + NROW, :] = mid
                m_buf[lo : lo + NROW, :] = rms(mid.astype(F32), gains[layer * 4 + 2])

        def mlp(lo):
            normed_mid = m_buf[...]
            gate = dot(normed_mid, w_gu[layer, :, lo : lo + FCH]).astype(BF).astype(F32)
            up = dot(normed_mid, w_gu[layer, :, FFN + lo : FFN + lo + FCH]).astype(BF).astype(F32)
            inner = gate * (0.7978845608028654 + (0.7978845608028654 * 0.044715) * (gate * gate))
            h_buf[:, lo : lo + FCH] = ((0.5 * gate) * (1.0 + jnp.tanh(inner)) * up).astype(BF)

        def down(lo):
            d_buf[:, lo : lo + NCH[lo]] = dot(h_buf[...], w_d[layer, :, lo : lo + NCH[lo]]).astype(BF)

        return project, norms, mlp, down

    def last(k):
        _, layer, piece, row = unit(jnp.maximum(k, 0))
        slot = jnp.where(k < 0, ROWS * NCP, row * NCP + piece)
        for lo in range(0, BLK, NROW):
            delta = rms(d_buf[lo : lo + NROW, :].astype(F32), gains[layer * 4 + 3])
            part = mid_buf[lo : lo + NROW, :].astype(F32)
            x_buf[slot, lo : lo + NROW, :] = (part + delta.astype(F32)).astype(BF)

    def attend_alone(k, count):
        key_value, query, score, mix = attend(k, count)
        key_value()
        for head in range(HEADS):
            query(head)
        for head in range(HEADS):
            for j in range(count):
                score(head, j)
        for head in range(HEADS):
            mix(head)

    def finish_alone(k):
        project, norms, mlp, down = finish(k)
        for lo in NCH:
            project(lo)
        norms()
        for lo in range(0, FFN, FCH):
            mlp(lo)
        for lo in NCH:
            down(lo)

    def together(k, count):
        key_value, query, score, mix = attend(k + 1, count)
        project, norms, mlp, down = finish(k)
        stream, layer, _, _ = unit(k + 1)
        for lo in NCH:
            project(lo)
        last(k - 1)
        enter(k + 1)
        rope(stream, (k + 1) // 4 + 1, layer)
        norms()
        key_value()
        for head in range(HEADS):
            query(head)
        softmax = []
        for head in range(HEADS):
            softmax += [functools.partial(score, head, j) for j in range(count)]
            if head > 0:
                softmax.append(functools.partial(mix, head - 1))
        softmax.append(functools.partial(mix, HEADS - 1))
        dense = [functools.partial(mlp, lo) for lo in range(0, FFN, FCH)] + [functools.partial(down, lo) for lo in NCH]
        order = [((i + 0.5) / len(softmax), f) for i, f in enumerate(softmax)]
        order += [((i + 0.5) / len(dense), f) for i, f in enumerate(dense)]
        for _, stage in sorted(order, key=lambda pair: pair[0]):
            stage()

    def hand_back(k):
        _, layer, piece, row = unit(k)

        @pl.when((layer == 1) & (piece == me))
        def _():
            own_out(row).start()

        @pl.when((layer == 1) & (piece != me))
        def _():
            send_out(row, piece).start()

    d_buf[...] = jnp.zeros((BLK, DIM), BF)
    mid_buf[...] = jnp.zeros((BLK, DIM), BF)
    for stream in range(2):
        for half in range(2):
            rope(stream, 0, half)
    rope(0, 1, 0)
    for copy in weight_copies(0)[:3]:
        copy.wait()
    receive(0)
    enter(0)
    attend_alone(0, 1)
    for copy in weight_copies(0)[3:]:
        copy.wait()

    def step(k, carry):
        after = k + 1
        stream, layer, piece, row = unit(after)

        @pl.when((k == 1) & (core == 1))
        def _():
            for r in range(2):
                send_piece(r, far_0).start()
                send_piece(r, far_1).start()

        @pl.when((piece == 1) & (layer == 0) & (row < ROWS - 2))
        def _():
            for dest in (partner, far_0, far_1):
                send_piece(row + 2, dest).start()

        @pl.when(k == 1)
        def _():
            for copy in weight_copies(1):
                copy.wait()

        @pl.when(layer == 0)
        def _():
            receive(after)

        blocks = jnp.where(layer == 0, jnp.minimum(piece, 2), piece) + 1
        for count in range(1, NCP + 1):
            @pl.when(blocks == count)
            def _():
                together(k, count)

        @pl.when(k > 0)
        def _():
            hand_back(k - 1)

        return carry

    lax.fori_loop(0, UNITS - 1, step, 0)
    last(UNITS - 2)
    hand_back(UNITS - 2)
    finish_alone(UNITS - 1)
    last(UNITS - 1)
    hand_back(UNITS - 1)

    for shift in range(1, NCP):
        other = peer(shift)
        send_pos(other).wait_send()
        for row in range(ROWS):
            send_piece(row, other).wait_send()
            send_out(row, other).wait_send()
            place = out.at[other * ROWS + row]
            pltpu.make_async_copy(place, place, out_recv.at[other * ROWS + row]).wait()
    for row in range(ROWS):
        own_out(row).wait()


def device_step(hidden, positions, *params):
    local_w, global_w = params[:11], params[11:]
    table = jnp.asarray(rope_lookup())
    hbm = pl.BlockSpec(memory_space=pltpu.HBM)
    vmem = pl.BlockSpec(memory_space=pltpu.VMEM)
    dma = pltpu.SemaphoreType.DMA
    return pl.pallas_call(
        kernel,
        out_shape=jax.ShapeDtypeStruct(hidden.shape, hidden.dtype),
        in_specs=[hbm, hbm, vmem] + [vmem] * 8 + [hbm] * 14,
        out_specs=pl.BlockSpec(memory_space=pl.ANY),
        scratch_shapes=[
            pltpu.VMEM((ROWS * NCP + 1, BLK, DIM), BF),
            pltpu.VMEM((NCP, NCP * ROWS, BLK), jnp.int32),
            pltpu.VMEM((2, DIM, QKV), BF),
            pltpu.VMEM((2, HEADS * HD, DIM), BF),
            pltpu.VMEM((2, DIM, 2 * FFN), BF),
            pltpu.VMEM((2, FFN, DIM), BF),
            pltpu.VMEM((2, 2, NCP * BLK, HD), BF),
            pltpu.VMEM((2, 2, NCP * BLK, HD), BF),
            pltpu.VMEM((HEADS, BLK, HD), BF),
            pltpu.VMEM((2, BLK, HEADS * HD), BF),
            pltpu.VMEM((HEADS, BLK, NCP * BLK), F32),
            pltpu.VMEM((BLK, FFN), BF),
            pltpu.VMEM((BLK, DIM), BF),
            pltpu.VMEM((BLK, DIM), BF),
            pltpu.VMEM((BLK, DIM), BF),
            pltpu.VMEM((BLK, DIM), BF),
            pltpu.VMEM((BLK, DIM), BF),
            pltpu.VMEM((4, BLK, HALF), F32),
            pltpu.VMEM((4, BLK, HALF), F32),
            pltpu.VMEM((4, BLK, 128), F32),
            pltpu.VMEM((8, 8, DIM), F32),
            dma((2, 7)),
            dma((ROWS, NCP)),
            dma((ROWS * NCP,)),
            dma((NCP,)),
            dma((NCP,)),
            dma((ROWS, NCP)),
            dma((NCP * ROWS,)),
        ],
        compiler_params=pltpu.CompilerParams(
            collective_id=0, has_side_effects=True, vmem_limit_bytes=67043328
        ),
        name="layers",
    )(hidden, positions, table, *local_w[7:], *global_w[7:], *local_w[:7], *global_w[:7])


def solution(mesh):
    specs_in = tuple([P("dp", "cp"), P("dp", "cp")] + [P()] * 22)
    return jax.shard_map(device_step, mesh=mesh, in_specs=specs_in, out_specs=P("dp", "cp"), check_vma=False)
```

```python
import functools

import jax
import jax.numpy as jnp
import numpy as np
from jax import lax
from jax.experimental import pallas as pl
from jax.experimental.pallas import tpu as pltpu
from jax.sharding import PartitionSpec as P

DIM = 640
HEADS = 4
HD = 256
HALF = HD // 2
FFN = 2048
WINDOW = 512
EPSILON = 1e-6
THETA = 10000.0
SOFT_CAP = 50.0
LOG2E = 1.4426950408889634
BLK = 256
NCP = 4
ROWS = 4
UNITS = ROWS * NCP * 2
QKV = HEADS * HD + 2 * HD
FCH = 256
NROW = 64
NCH = {0: 256, 256: 256, 512: 128}
LOW = 64
HIGH = 32
BF = jnp.bfloat16
F32 = jnp.float32
MESH = pl.DeviceIdType.MESH


def rope_lookup():
    inv_freq = THETA ** (-(np.arange(HALF, dtype=np.float64) * 2.0 / HD))
    table = np.zeros((128, 4 * HALF), np.float64)
    high = np.arange(HIGH)[:, None] * float(LOW) * inv_freq
    low = np.arange(LOW)[:, None] * inv_freq
    table[:HIGH, 0:HALF] = np.cos(high)
    table[:HIGH, HALF : 2 * HALF] = np.sin(high)
    table[HIGH : HIGH + LOW, 2 * HALF : 3 * HALF] = np.cos(low)
    table[HIGH : HIGH + LOW, 3 * HALF :] = np.sin(low)
    parts = []
    rest = table
    for _ in range(3):
        part = rest.astype(jnp.bfloat16)
        parts.append(part)
        rest = rest - part.astype(np.float64)
    return np.concatenate(parts, axis=0)


def dot(lhs, rhs):
    return jnp.dot(lhs, rhs, preferred_element_type=F32)


def rms(wide, gain):
    mean_sq = jnp.mean(wide * wide, axis=-1, keepdims=True)
    tall = (wide * lax.rsqrt(mean_sq + EPSILON)).reshape(-1, 8, DIM) * gain[None]
    return tall.reshape(-1, DIM).astype(BF)


def unit(k):
    stream = lax.rem(k, 2)
    turn = k // 2
    layer = lax.rem(turn, 2)
    piece = lax.rem(turn // 2, NCP)
    row = (turn // (2 * NCP)) * 2 + stream
    return stream, layer, piece, row


def kernel(hid, pos, table, *rest):
    scales = rest[:8]
    weights = rest[8:22]
    out = rest[22]
    (x_buf, pos_buf, w_qkv, w_o, w_gu, w_d, k_buf, v_buf, q_buf, o_buf, e_buf, h_buf, a_buf, m_buf, t_buf, d_buf, mid_buf, cos_buf,
     sin_buf, qp_buf, gains, w_sem, in_send, in_recv, pos_send, pos_recv, out_send, out_recv) = rest[23:]
    me = lax.axis_index("cp")

    def weight_copies(layer):
        w_q, w_k, w_v, wo, wg, wu, wd = weights[7 * layer : 7 * layer + 7]
        places = (
            (w_q, w_qkv.at[layer, :, 0:1024]),
            (w_k, w_qkv.at[layer, :, 1024:1280]),
            (w_v, w_qkv.at[layer, :, 1280:1536]),
            (wo, w_o.at[layer]),
            (wg, w_gu.at[layer, :, 0:FFN]),
            (wu, w_gu.at[layer, :, FFN : 2 * FFN]),
            (wd, w_d.at[layer]),
        )
        return [pltpu.make_async_copy(src, dst, w_sem.at[layer, i]) for i, (src, dst) in enumerate(places)]

    def peer(shift):
        return lax.rem(me + shift, NCP)

    def send_piece(row, dest):
        return pltpu.make_async_remote_copy(
            src_ref=hid.at[dest * ROWS + row],
            dst_ref=x_buf.at[row * NCP + me],
            send_sem=in_send.at[row, dest],
            recv_sem=in_recv.at[row * NCP + me],
            device_id={"cp": dest},
            device_id_type=MESH,
        )

    def own_piece(row):
        return pltpu.make_async_copy(hid.at[me * ROWS + row], x_buf.at[row * NCP + me], in_recv.at[row * NCP + me])

    def send_pos(dest):
        return pltpu.make_async_remote_copy(
            src_ref=pos,
            dst_ref=pos_buf.at[me],
            send_sem=pos_send.at[dest],
            recv_sem=pos_recv.at[me],
            device_id={"cp": dest},
            device_id_type=MESH,
        )

    def own_pos():
        return pltpu.make_async_copy(pos, pos_buf.at[me], pos_recv.at[me])

    def send_out(row, piece):
        return pltpu.make_async_remote_copy(
            src_ref=x_buf.at[row * NCP + piece],
            dst_ref=out.at[me * ROWS + row],
            send_sem=out_send.at[row, piece],
            recv_sem=out_recv.at[me * ROWS + row],
            device_id={"cp": piece},
            device_id_type=MESH,
        )

    def own_out(row):
        return pltpu.make_async_copy(x_buf.at[row * NCP + me], out.at[me * ROWS + row], out_send.at[row, me])

    for copy in weight_copies(0)[:3]:
        copy.start()
    own_piece(0).start()
    own_pos().start()
    own_piece(1).start()

    barrier = pltpu.get_barrier_semaphore()
    for shift in range(1, NCP):
        pl.semaphore_signal(barrier, inc=1, device_id={"cp": peer(shift)}, device_id_type=MESH)
    pl.semaphore_wait(barrier, NCP - 1)

    core = lax.rem(me, 2)
    partner = me + 1 - 2 * core
    far_0 = lax.rem(me + 2 - core, NCP)
    far_1 = lax.rem(me + 3 - core, NCP)
    for shift in range(1, NCP):
        send_pos(peer(shift)).start()
    for row in range(2):
        send_piece(row, partner).start()

    @pl.when(core == 0)
    def _():
        for row in range(2):
            send_piece(row, far_0).start()
            send_piece(row, far_1).start()

    for copy in weight_copies(0)[3:] + weight_copies(1):
        copy.start()
    for row in range(2, ROWS):
        own_piece(row).start()
    for i in range(8):
        gains[i] = jnp.broadcast_to(1.0 + scales[i][...].reshape(1, DIM), (8, DIM))
    own_pos().wait()
    for shift in range(1, NCP):
        src = peer(shift)
        pltpu.make_async_copy(pos_buf.at[src], pos_buf.at[src], pos_recv.at[src]).wait()

    def positions_of(piece, row):
        return pos_buf[piece, pl.ds(me * ROWS + row, 1), :].astype(F32)

    def receive(k):
        _, _, piece, row = unit(k)
        x_ref = x_buf.at[row * NCP + piece]
        pltpu.make_async_copy(x_ref, x_ref, in_recv.at[row * NCP + piece]).wait()

    def rope(stream, index, half):
        piece = lax.rem(index, NCP)
        row = jnp.minimum(index // NCP, 1) * 2 + stream
        slot = stream * 2 + lax.rem(index, 2)
        spot = pl.multiple_of(half * 128, 128)
        whole_row = positions_of(piece, row)
        row_pos = jnp.where(half == 0, whole_row[:, :128], whole_row[:, 128:])
        col_pos = jnp.transpose(jnp.broadcast_to(row_pos, (128, 128)))
        whole = col_pos.astype(jnp.int32)
        lane = lax.broadcasted_iota(jnp.int32, (128, 128), 1)
        hit = jnp.where((lane == (whole >> 6)) | (lane == (whole & (LOW - 1)) + HIGH), 1.0, 0.0).astype(BF)
        found = dot(jnp.concatenate([hit, hit], axis=1), table[0:256, :]) + dot(hit, table[256:384, :])
        c_hi, s_hi = found[:, 0:HALF], found[:, HALF : 2 * HALF]
        c_lo, s_lo = found[:, 2 * HALF : 3 * HALF], found[:, 3 * HALF :]
        qp_buf[slot, pl.ds(spot, 128), :] = col_pos
        cos_buf[slot, pl.ds(spot, 128), :] = c_hi * c_lo - s_hi * s_lo
        sin_buf[slot, pl.ds(spot, 128), :] = s_hi * c_lo + c_hi * s_lo

    def enter(k):
        _, layer, piece, row = unit(k)
        for lo in range(0, BLK, NROW):
            part = x_buf[row * NCP + piece, lo : lo + NROW, :].astype(F32)
            a_buf[lo : lo + NROW, :] = rms(part, gains[layer * 4])

    def attend(k, count):
        stream, layer, piece, row = unit(k)
        turn = stream * 2 + lax.rem(piece, 2)
        cos_t, sin_t = cos_buf[turn], sin_buf[turn]
        spot = pl.multiple_of(piece * BLK, BLK)
        keys = count * BLK
        first = piece - (count - 1)
        base = pl.multiple_of(first * BLK, BLK)
        below = lax.broadcasted_iota(jnp.int32, (128, 128), 0) >= lax.broadcasted_iota(jnp.int32, (128, 128), 1)
        window = jnp.where(layer == 0, float(WINDOW), 65536.0)
        q_low = qp_buf[turn] - window
        totals = {}

        def rotate(raw):
            wide = raw.astype(BF).astype(F32)
            one, two = wide[:, :HALF], wide[:, HALF:]
            return one * cos_t - two * sin_t, two * cos_t + one * sin_t

        def key_value():
            normed = a_buf[...]
            one, two = rotate(dot(normed, w_qkv[layer, :, 1024:1280]))
            k_buf[stream, layer, pl.ds(spot, BLK), :HALF] = one.astype(BF)
            k_buf[stream, layer, pl.ds(spot, BLK), HALF:] = two.astype(BF)
            v_buf[stream, layer, pl.ds(spot, BLK), :] = dot(normed, w_qkv[layer, :, 1280:1536]).astype(BF)

        def query(head):
            one, two = rotate(dot(a_buf[...], w_qkv[layer, :, head * HD : (head + 1) * HD]))
            q_buf[head, :, :HALF] = (one * HD**-0.5).astype(BF)
            q_buf[head, :, HALF:] = (two * HD**-0.5).astype(BF)

        def weigh(raw):
            return jnp.exp2(jnp.tanh(raw * (1.0 / SOFT_CAP)) * (SOFT_CAP * LOG2E))

        def score(head, j):
            key = k_buf[stream, layer, pl.ds(base + j * BLK, BLK), :]
            raw = lax.dot_general(q_buf[head], key, (((1,), (1,)), ((), ())), preferred_element_type=F32)
            if j == count - 1:
                early = jnp.where(below, weigh(raw[:128, :128]), 0.0)
                late = weigh(raw[128:, :128])
                rest = jnp.where(below, weigh(raw[128:, 128:]), 0.0)
                e_buf[head, :128, j * BLK : j * BLK + 128] = early
                e_buf[head, 128:, j * BLK : j * BLK + 128] = late
                e_buf[head, :128, j * BLK + 128 : (j + 1) * BLK] = jnp.zeros((128, 128), F32)
                e_buf[head, 128:, j * BLK + 128 : (j + 1) * BLK] = rest
                part = jnp.concatenate([early, late + rest], axis=0)
            else:
                soft = weigh(raw)
                if count < NCP:
                    k_pos = positions_of(first + j, row)
                    halves = []
                    for lo in (0, 128):
                        halves.append(jnp.where(q_low < k_pos[:, lo : lo + 128], soft[:, lo : lo + 128], 0.0))
                    soft = jnp.concatenate(halves, axis=1)
                e_buf[head, :, j * BLK : (j + 1) * BLK] = soft
                part = soft[:, :128] + soft[:, 128:]
            totals[head] = part if j == 0 else totals[head] + part
            if j == count - 1:
                totals[head] = 1.0 / jnp.sum(totals[head], axis=-1, keepdims=True)

        def mix(head):
            prob = (e_buf[head, :, 0:keys] * totals[head]).astype(BF)
            mixed = dot(prob, v_buf[stream, layer, pl.ds(base, keys), :])
            o_buf[stream, :, head * HD : (head + 1) * HD] = mixed.astype(BF)

        return key_value, query, score, mix

    def finish(k):
        stream, layer, piece, row = unit(k)
        kept = {}

        def project(lo):
            t_buf[:, lo : lo + NCH[lo]] = dot(o_buf[stream], w_o[layer, :, lo : lo + NCH[lo]]).astype(BF)

        def norms():
            for lo in range(0, BLK, NROW):
                delta = rms(t_buf[lo : lo + NROW, :].astype(F32), gains[layer * 4 + 1])
                part = x_buf[row * NCP + piece, lo : lo + NROW, :].astype(F32)
                mid = (part + delta.astype(F32)).astype(BF)
                mid_buf[lo : lo + NROW, :] = mid
                m_buf[lo : lo + NROW, :] = rms(mid.astype(F32), gains[layer * 4 + 2])

        def mlp(lo):
            normed_mid = m_buf[...]
            gate = dot(normed_mid, w_gu[layer, :, lo : lo + FCH]).astype(BF).astype(F32)
            up = dot(normed_mid, w_gu[layer, :, FFN + lo : FFN + lo + FCH]).astype(BF).astype(F32)
            inner = gate * (0.7978845608028654 + (0.7978845608028654 * 0.044715) * (gate * gate))
            h_buf[:, lo : lo + FCH] = ((0.5 * gate) * (1.0 + jnp.tanh(inner)) * up).astype(BF)

        def down(lo):
            d_buf[:, lo : lo + NCH[lo]] = dot(h_buf[...], w_d[layer, :, lo : lo + NCH[lo]]).astype(BF)

        return project, norms, mlp, down

    def last(k):
        _, layer, piece, row = unit(jnp.maximum(k, 0))
        slot = jnp.where(k < 0, ROWS * NCP, row * NCP + piece)
        for lo in range(0, BLK, NROW):
            delta = rms(d_buf[lo : lo + NROW, :].astype(F32), gains[layer * 4 + 3])
            part = mid_buf[lo : lo + NROW, :].astype(F32)
            x_buf[slot, lo : lo + NROW, :] = (part + delta.astype(F32)).astype(BF)

    def attend_alone(k, count):
        key_value, query, score, mix = attend(k, count)
        key_value()
        for head in range(HEADS):
            query(head)
        for head in range(HEADS):
            for j in range(count):
                score(head, j)
        for head in range(HEADS):
            mix(head)

    def finish_alone(k):
        project, norms, mlp, down = finish(k)
        for lo in NCH:
            project(lo)
        norms()
        for lo in range(0, FFN, FCH):
            mlp(lo)
        for lo in NCH:
            down(lo)

    def together(k, count):
        key_value, query, score, mix = attend(k + 1, count)
        project, norms, mlp, down = finish(k)
        stream, layer, _, _ = unit(k + 1)
        for lo in NCH:
            project(lo)
        last(k - 1)
        enter(k + 1)
        rope(stream, (k + 1) // 4 + 1, layer)
        norms()
        key_value()
        for head in range(HEADS):
            query(head)
        softmax = []
        for head in range(HEADS):
            softmax += [functools.partial(score, head, j) for j in range(count)]
            if head > 0:
                softmax.append(functools.partial(mix, head - 1))
        softmax.append(functools.partial(mix, HEADS - 1))
        dense = [functools.partial(mlp, lo) for lo in range(0, FFN, FCH)] + [functools.partial(down, lo) for lo in NCH]
        order = [((i + 0.5) / len(softmax), f) for i, f in enumerate(softmax)]
        order += [((i + 0.5) / len(dense), f) for i, f in enumerate(dense)]
        for _, stage in sorted(order, key=lambda pair: pair[0]):
            stage()

    def hand_back(k):
        _, layer, piece, row = unit(k)

        @pl.when((layer == 1) & (piece == me))
        def _():
            own_out(row).start()

        @pl.when((layer == 1) & (piece != me))
        def _():
            send_out(row, piece).start()

    d_buf[...] = jnp.zeros((BLK, DIM), BF)
    mid_buf[...] = jnp.zeros((BLK, DIM), BF)
    for stream in range(2):
        for half in range(2):
            rope(stream, 0, half)
    rope(0, 1, 0)
    for copy in weight_copies(0)[:3]:
        copy.wait()
    receive(0)
    enter(0)
    attend_alone(0, 1)
    for copy in weight_copies(0)[3:]:
        copy.wait()

    def step(k, carry):
        after = k + 1
        stream, layer, piece, row = unit(after)

        @pl.when((k == 1) & (core == 1))
        def _():
            for r in range(2):
                send_piece(r, far_0).start()
                send_piece(r, far_1).start()

        @pl.when((piece == 1) & (layer == 0) & (row < ROWS - 2))
        def _():
            for dest in (partner, far_0, far_1):
                send_piece(row + 2, dest).start()

        @pl.when(k == 1)
        def _():
            for copy in weight_copies(1):
                copy.wait()

        @pl.when(layer == 0)
        def _():
            receive(after)

        blocks = jnp.where(layer == 0, jnp.minimum(piece, 2), piece) + 1
        for count in range(1, NCP + 1):
            @pl.when(blocks == count)
            def _():
                together(k, count)

        @pl.when(k > 0)
        def _():
            hand_back(k - 1)

        return carry

    lax.fori_loop(0, UNITS - 1, step, 0)
    last(UNITS - 2)
    hand_back(UNITS - 2)
    finish_alone(UNITS - 1)
    last(UNITS - 1)
    hand_back(UNITS - 1)

    for shift in range(1, NCP):
        other = peer(shift)
        send_pos(other).wait_send()
        for row in range(ROWS):
            send_piece(row, other).wait_send()
            send_out(row, other).wait_send()
            place = out.at[other * ROWS + row]
            pltpu.make_async_copy(place, place, out_recv.at[other * ROWS + row]).wait()
    for row in range(ROWS):
        own_out(row).wait()


def device_step(hidden, positions, *params):
    local_w, global_w = params[:11], params[11:]
    table = jnp.asarray(rope_lookup())
    hbm = pl.BlockSpec(memory_space=pltpu.HBM)
    vmem = pl.BlockSpec(memory_space=pltpu.VMEM)
    dma = pltpu.SemaphoreType.DMA
    mixed = pl.pallas_call(
        kernel,
        out_shape=jax.ShapeDtypeStruct(hidden.shape, hidden.dtype),
        in_specs=[hbm, hbm, vmem] + [vmem] * 8 + [hbm] * 14,
        out_specs=pl.BlockSpec(memory_space=pl.ANY),
        scratch_shapes=[
            pltpu.VMEM((ROWS * NCP + 1, BLK, DIM), BF),
            pltpu.VMEM((NCP, NCP * ROWS, BLK), jnp.int32),
            pltpu.VMEM((2, DIM, QKV), BF),
            pltpu.VMEM((2, HEADS * HD, DIM), BF),
            pltpu.VMEM((2, DIM, 2 * FFN), BF),
            pltpu.VMEM((2, FFN, DIM), BF),
            pltpu.VMEM((2, 2, NCP * BLK, HD), BF),
            pltpu.VMEM((2, 2, NCP * BLK, HD), BF),
            pltpu.VMEM((HEADS, BLK, HD), BF),
            pltpu.VMEM((2, BLK, HEADS * HD), BF),
            pltpu.VMEM((HEADS, BLK, NCP * BLK), F32),
            pltpu.VMEM((BLK, FFN), BF),
            pltpu.VMEM((BLK, DIM), BF),
            pltpu.VMEM((BLK, DIM), BF),
            pltpu.VMEM((BLK, DIM), BF),
            pltpu.VMEM((BLK, DIM), BF),
            pltpu.VMEM((BLK, DIM), BF),
            pltpu.VMEM((4, BLK, HALF), F32),
            pltpu.VMEM((4, BLK, HALF), F32),
            pltpu.VMEM((4, BLK, 128), F32),
            pltpu.VMEM((8, 8, DIM), F32),
            dma((2, 7)),
            dma((ROWS, NCP)),
            dma((ROWS * NCP,)),
            dma((NCP,)),
            dma((NCP,)),
            dma((ROWS, NCP)),
            dma((NCP * ROWS,)),
        ],
        compiler_params=pltpu.CompilerParams(
            collective_id=0, has_side_effects=True, vmem_limit_bytes=67043328
        ),
        name="layers",
    )(hidden, positions, table, *local_w[7:], *global_w[7:], *local_w[:7], *global_w[:7])
    tile = pl.BlockSpec((2, BLK, DIM), lambda i: (i, 0, 0))
    return pl.pallas_call(
        lambda src, dst: dst.__setitem__(..., src[...]),
        out_shape=jax.ShapeDtypeStruct(hidden.shape, hidden.dtype),
        grid=(hidden.shape[0] // 2,),
        in_specs=[tile],
        out_specs=tile,
        name="settle",
    )(mixed)


def solution(mesh):
    specs_in = tuple([P("dp", "cp"), P("dp", "cp")] + [P()] * 22)
    return jax.shard_map(device_step, mesh=mesh, in_specs=specs_in, out_specs=P("dp", "cp"), check_vma=False)
```

```python
import functools

import jax
import jax.numpy as jnp
import numpy as np
from jax import lax
from jax.experimental import pallas as pl
from jax.experimental.pallas import tpu as pltpu
from jax.sharding import PartitionSpec as P

DIM = 640
HEADS = 4
HD = 256
HALF = HD // 2
FFN = 2048
WINDOW = 512
EPSILON = 1e-6
THETA = 10000.0
SOFT_CAP = 50.0
LOG2E = 1.4426950408889634
BLK = 256
NCP = 4
ROWS = 4
UNITS = ROWS * NCP * 2
QKV = HEADS * HD + 2 * HD
FCH = 256
NROW = 64
NCH = {0: 256, 256: 256, 512: 128}
LOW = 64
HIGH = 32
BF = jnp.bfloat16
F32 = jnp.float32
MESH = pl.DeviceIdType.MESH


def rope_lookup():
    inv_freq = THETA ** (-(np.arange(HALF, dtype=np.float64) * 2.0 / HD))
    table = np.zeros((128, 4 * HALF), np.float64)
    high = np.arange(HIGH)[:, None] * float(LOW) * inv_freq
    low = np.arange(LOW)[:, None] * inv_freq
    table[:HIGH, 0:HALF] = np.cos(high)
    table[:HIGH, HALF : 2 * HALF] = np.sin(high)
    table[HIGH : HIGH + LOW, 2 * HALF : 3 * HALF] = np.cos(low)
    table[HIGH : HIGH + LOW, 3 * HALF :] = np.sin(low)
    parts = []
    rest = table
    for _ in range(3):
        part = rest.astype(jnp.bfloat16)
        parts.append(part)
        rest = rest - part.astype(np.float64)
    return np.concatenate(parts, axis=0)


def dot(lhs, rhs):
    return jnp.dot(lhs, rhs, preferred_element_type=F32)


def rms(wide, gain):
    mean_sq = jnp.mean(wide * wide, axis=-1, keepdims=True)
    tall = (wide * lax.rsqrt(mean_sq + EPSILON)).reshape(-1, 8, DIM) * gain[None]
    return tall.reshape(-1, DIM).astype(BF)


def unit(k):
    stream = lax.rem(k, 2)
    turn = k // 2
    layer = lax.rem(turn, 2)
    piece = lax.rem(turn // 2, NCP)
    row = (turn // (2 * NCP)) * 2 + stream
    return stream, layer, piece, row


def kernel(hid, pos, table, *rest):
    scales = rest[:8]
    weights = rest[8:22]
    out = rest[22]
    (x_buf, pos_buf, w_qkv, w_o, w_gu, w_d, k_buf, v_buf, q_buf, o_buf, e_buf, h_buf, a_buf, m_buf, t_buf, d_buf, mid_buf, cos_buf,
     sin_buf, qp_buf, gains, w_sem, in_send, in_recv, pos_send, pos_recv, out_send, out_recv) = rest[23:]
    me = lax.axis_index("cp")

    def weight_copies(layer):
        w_q, w_k, w_v, wo, wg, wu, wd = weights[7 * layer : 7 * layer + 7]
        places = (
            (w_q, w_qkv.at[layer, :, 0:1024]),
            (w_k, w_qkv.at[layer, :, 1024:1280]),
            (w_v, w_qkv.at[layer, :, 1280:1536]),
            (wo, w_o.at[layer]),
            (wg, w_gu.at[layer, :, 0:FFN]),
            (wu, w_gu.at[layer, :, FFN : 2 * FFN]),
            (wd, w_d.at[layer]),
        )
        return [pltpu.make_async_copy(src, dst, w_sem.at[layer, i]) for i, (src, dst) in enumerate(places)]

    def peer(shift):
        return lax.rem(me + shift, NCP)

    def send_piece(row, dest):
        return pltpu.make_async_remote_copy(
            src_ref=hid.at[dest * ROWS + row],
            dst_ref=x_buf.at[row * NCP + me],
            send_sem=in_send.at[row, dest],
            recv_sem=in_recv.at[row * NCP + me],
            device_id={"cp": dest},
            device_id_type=MESH,
        )

    def own_piece(row):
        return pltpu.make_async_copy(hid.at[me * ROWS + row], x_buf.at[row * NCP + me], in_recv.at[row * NCP + me])

    def send_pos(dest):
        return pltpu.make_async_remote_copy(
            src_ref=pos,
            dst_ref=pos_buf.at[me],
            send_sem=pos_send.at[dest],
            recv_sem=pos_recv.at[me],
            device_id={"cp": dest},
            device_id_type=MESH,
        )

    def own_pos():
        return pltpu.make_async_copy(pos, pos_buf.at[me], pos_recv.at[me])

    def send_out(row, piece):
        return pltpu.make_async_remote_copy(
            src_ref=x_buf.at[row * NCP + piece],
            dst_ref=out.at[me * ROWS + row],
            send_sem=out_send.at[row, piece],
            recv_sem=out_recv.at[me * ROWS + row],
            device_id={"cp": piece},
            device_id_type=MESH,
        )

    def own_out(row):
        return pltpu.make_async_copy(x_buf.at[row * NCP + me], out.at[me * ROWS + row], out_send.at[row, me])

    for copy in weight_copies(0)[:3]:
        copy.start()
    own_piece(0).start()
    own_pos().start()
    own_piece(1).start()

    barrier = pltpu.get_barrier_semaphore()
    for shift in range(1, NCP):
        pl.semaphore_signal(barrier, inc=1, device_id={"cp": peer(shift)}, device_id_type=MESH)
    pl.semaphore_wait(barrier, NCP - 1)

    core = lax.rem(me, 2)
    partner = me + 1 - 2 * core
    far_0 = lax.rem(me + 2 - core, NCP)
    far_1 = lax.rem(me + 3 - core, NCP)
    for shift in range(1, NCP):
        send_pos(peer(shift)).start()
    for row in range(2):
        send_piece(row, partner).start()

    @pl.when(core == 0)
    def _():
        for row in range(2):
            send_piece(row, far_0).start()
            send_piece(row, far_1).start()

    for copy in weight_copies(0)[3:] + weight_copies(1):
        copy.start()
    for row in range(2, ROWS):
        own_piece(row).start()
    for i in range(8):
        gains[i] = jnp.broadcast_to(1.0 + scales[i][...].reshape(1, DIM), (8, DIM))
    own_pos().wait()
    for shift in range(1, NCP):
        src = peer(shift)
        pltpu.make_async_copy(pos_buf.at[src], pos_buf.at[src], pos_recv.at[src]).wait()

    def positions_of(piece, row):
        return pos_buf[piece, pl.ds(me * ROWS + row, 1), :].astype(F32)

    def receive(k):
        _, _, piece, row = unit(k)
        x_ref = x_buf.at[row * NCP + piece]
        pltpu.make_async_copy(x_ref, x_ref, in_recv.at[row * NCP + piece]).wait()

    def rope(stream, index, half):
        piece = lax.rem(index, NCP)
        row = jnp.minimum(index // NCP, 1) * 2 + stream
        slot = stream * 2 + lax.rem(index, 2)
        spot = pl.multiple_of(half * 128, 128)
        whole_row = positions_of(piece, row)
        row_pos = jnp.where(half == 0, whole_row[:, :128], whole_row[:, 128:])
        col_pos = jnp.transpose(jnp.broadcast_to(row_pos, (128, 128)))
        whole = col_pos.astype(jnp.int32)
        lane = lax.broadcasted_iota(jnp.int32, (128, 128), 1)
        hit = jnp.where((lane == (whole >> 6)) | (lane == (whole & (LOW - 1)) + HIGH), 1.0, 0.0).astype(BF)
        found = dot(jnp.concatenate([hit, hit], axis=1), table[0:256, :]) + dot(hit, table[256:384, :])
        c_hi, s_hi = found[:, 0:HALF], found[:, HALF : 2 * HALF]
        c_lo, s_lo = found[:, 2 * HALF : 3 * HALF], found[:, 3 * HALF :]
        qp_buf[slot, pl.ds(spot, 128), :] = col_pos
        cos_buf[slot, pl.ds(spot, 128), :] = c_hi * c_lo - s_hi * s_lo
        sin_buf[slot, pl.ds(spot, 128), :] = s_hi * c_lo + c_hi * s_lo

    def enter(k):
        _, layer, piece, row = unit(k)
        for lo in range(0, BLK, NROW):
            part = x_buf[row * NCP + piece, lo : lo + NROW, :].astype(F32)
            a_buf[lo : lo + NROW, :] = rms(part, gains[layer * 4])

    def attend(k, count):
        stream, layer, piece, row = unit(k)
        turn = stream * 2 + lax.rem(piece, 2)
        cos_t, sin_t = cos_buf[turn], sin_buf[turn]
        spot = pl.multiple_of(piece * BLK, BLK)
        keys = count * BLK
        first = piece - (count - 1)
        base = pl.multiple_of(first * BLK, BLK)
        below = lax.broadcasted_iota(jnp.int32, (128, 128), 0) >= lax.broadcasted_iota(jnp.int32, (128, 128), 1)
        window = jnp.where(layer == 0, float(WINDOW), 65536.0)
        q_low = qp_buf[turn] - window
        totals = {}

        def rotate(raw):
            wide = raw.astype(BF).astype(F32)
            one, two = wide[:, :HALF], wide[:, HALF:]
            return one * cos_t - two * sin_t, two * cos_t + one * sin_t

        def key_value():
            normed = a_buf[...]
            one, two = rotate(dot(normed, w_qkv[layer, :, 1024:1280]))
            k_buf[stream, layer, pl.ds(spot, BLK), :HALF] = one.astype(BF)
            k_buf[stream, layer, pl.ds(spot, BLK), HALF:] = two.astype(BF)
            v_buf[stream, layer, pl.ds(spot, BLK), :] = dot(normed, w_qkv[layer, :, 1280:1536]).astype(BF)

        def query(head):
            one, two = rotate(dot(a_buf[...], w_qkv[layer, :, head * HD : (head + 1) * HD]))
            q_buf[head, :, :HALF] = (one * HD**-0.5).astype(BF)
            q_buf[head, :, HALF:] = (two * HD**-0.5).astype(BF)

        def weigh(raw):
            return jnp.exp2(jnp.tanh(raw * (1.0 / SOFT_CAP)) * (SOFT_CAP * LOG2E))

        def score(head, j):
            key = k_buf[stream, layer, pl.ds(base + j * BLK, BLK), :]
            raw = lax.dot_general(q_buf[head], key, (((1,), (1,)), ((), ())), preferred_element_type=F32)
            if j == count - 1:
                early = jnp.where(below, weigh(raw[:128, :128]), 0.0)
                late = weigh(raw[128:, :128])
                rest = jnp.where(below, weigh(raw[128:, 128:]), 0.0)
                e_buf[head, :128, j * BLK : j * BLK + 128] = early
                e_buf[head, 128:, j * BLK : j * BLK + 128] = late
                e_buf[head, :128, j * BLK + 128 : (j + 1) * BLK] = jnp.zeros((128, 128), F32)
                e_buf[head, 128:, j * BLK + 128 : (j + 1) * BLK] = rest
                part = jnp.concatenate([early, late + rest], axis=0)
            else:
                soft = weigh(raw)
                if count < NCP:
                    k_pos = positions_of(first + j, row)
                    halves = []
                    for lo in (0, 128):
                        halves.append(jnp.where(q_low < k_pos[:, lo : lo + 128], soft[:, lo : lo + 128], 0.0))
                    soft = jnp.concatenate(halves, axis=1)
                e_buf[head, :, j * BLK : (j + 1) * BLK] = soft
                part = soft[:, :128] + soft[:, 128:]
            totals[head] = part if j == 0 else totals[head] + part
            if j == count - 1:
                totals[head] = 1.0 / jnp.sum(totals[head], axis=-1, keepdims=True)

        def mix(head):
            prob = (e_buf[head, :, 0:keys] * totals[head]).astype(BF)
            mixed = dot(prob, v_buf[stream, layer, pl.ds(base, keys), :])
            o_buf[stream, :, head * HD : (head + 1) * HD] = mixed.astype(BF)

        return key_value, query, score, mix

    def finish(k):
        stream, layer, piece, row = unit(k)
        kept = {}

        def project(lo):
            t_buf[:, lo : lo + NCH[lo]] = dot(o_buf[stream], w_o[layer, :, lo : lo + NCH[lo]]).astype(BF)

        def norms():
            for lo in range(0, BLK, NROW):
                delta = rms(t_buf[lo : lo + NROW, :].astype(F32), gains[layer * 4 + 1])
                part = x_buf[row * NCP + piece, lo : lo + NROW, :].astype(F32)
                mid = (part + delta.astype(F32)).astype(BF)
                mid_buf[lo : lo + NROW, :] = mid
                m_buf[lo : lo + NROW, :] = rms(mid.astype(F32), gains[layer * 4 + 2])

        def mlp(lo):
            normed_mid = m_buf[...]
            gate = dot(normed_mid, w_gu[layer, :, lo : lo + FCH]).astype(BF).astype(F32)
            up = dot(normed_mid, w_gu[layer, :, FFN + lo : FFN + lo + FCH]).astype(BF).astype(F32)
            inner = gate * (0.7978845608028654 + (0.7978845608028654 * 0.044715) * (gate * gate))
            h_buf[:, lo : lo + FCH] = ((0.5 * gate) * (1.0 + jnp.tanh(inner)) * up).astype(BF)

        def down(lo):
            d_buf[:, lo : lo + NCH[lo]] = dot(h_buf[...], w_d[layer, :, lo : lo + NCH[lo]]).astype(BF)

        return project, norms, mlp, down

    def last(k):
        _, layer, piece, row = unit(jnp.maximum(k, 0))
        slot = jnp.where(k < 0, ROWS * NCP, row * NCP + piece)
        for lo in range(0, BLK, NROW):
            delta = rms(d_buf[lo : lo + NROW, :].astype(F32), gains[layer * 4 + 3])
            part = mid_buf[lo : lo + NROW, :].astype(F32)
            x_buf[slot, lo : lo + NROW, :] = (part + delta.astype(F32)).astype(BF)

    def attend_alone(k, count):
        key_value, query, score, mix = attend(k, count)
        key_value()
        for head in range(HEADS):
            query(head)
        for head in range(HEADS):
            for j in range(count):
                score(head, j)
        for head in range(HEADS):
            mix(head)

    def finish_alone(k):
        project, norms, mlp, down = finish(k)
        for lo in NCH:
            project(lo)
        norms()
        for lo in range(0, FFN, FCH):
            mlp(lo)
        for lo in NCH:
            down(lo)

    def together(k, count):
        key_value, query, score, mix = attend(k + 1, count)
        project, norms, mlp, down = finish(k)
        stream, layer, _, _ = unit(k + 1)
        for lo in NCH:
            project(lo)
        last(k - 1)
        enter(k + 1)
        rope(stream, (k + 1) // 4 + 1, layer)
        norms()
        key_value()
        for head in range(HEADS):
            query(head)
        softmax = []
        for head in range(HEADS):
            softmax += [functools.partial(score, head, j) for j in range(count)]
            if head > 0:
                softmax.append(functools.partial(mix, head - 1))
        softmax.append(functools.partial(mix, HEADS - 1))
        dense = [functools.partial(mlp, lo) for lo in range(0, FFN, FCH)] + [functools.partial(down, lo) for lo in NCH]
        order = [((i + 0.5) / len(softmax), f) for i, f in enumerate(softmax)]
        order += [((i + 0.5) / len(dense), f) for i, f in enumerate(dense)]
        for _, stage in sorted(order, key=lambda pair: pair[0]):
            stage()

    def hand_back(k):
        _, layer, piece, row = unit(k)

        @pl.when((layer == 1) & (piece == me))
        def _():
            own_out(row).start()

        @pl.when((layer == 1) & (piece != me))
        def _():
            send_out(row, piece).start()

    d_buf[...] = jnp.zeros((BLK, DIM), BF)
    mid_buf[...] = jnp.zeros((BLK, DIM), BF)
    for stream in range(2):
        for half in range(2):
            rope(stream, 0, half)
    for copy in weight_copies(0)[:3]:
        copy.wait()

    def step(k, carry):
        after = k + 1
        stream, layer, piece, row = unit(after)
        alone = (k == 0) & (me >= 2)
        opening = k < 0
        closing = k == UNITS - 1

        @pl.when(k == 0)
        def _():
            for copy in weight_copies(0)[3:]:
                copy.wait()

        @pl.when((k == 1) & (core == 1))
        def _():
            for r in range(2):
                send_piece(r, far_0).start()
                send_piece(r, far_1).start()

        @pl.when((piece == 1) & (layer == 0) & (row < ROWS - 2))
        def _():
            for dest in (partner, far_0, far_1):
                send_piece(row + 2, dest).start()

        @pl.when(k == 1)
        def _():
            for copy in weight_copies(1):
                copy.wait()

        @pl.when(alone | closing)
        def _():
            last(k - 1)

            @pl.when(closing)
            def _():
                hand_back(k - 1)

            finish_alone(k)
            last(k)

        @pl.when((layer == 0) & (k < UNITS - 1))
        def _():
            receive(after)

        @pl.when(alone | opening)
        def _():
            enter(after)
            attend_alone(after, 1)
            rope(stream, after // 4 + 1, layer)

        blocks = jnp.where(layer == 0, jnp.minimum(piece, 2), piece) + 1
        blocks = jnp.where(alone | opening | closing, 0, blocks)
        for count in range(1, NCP + 1):
            @pl.when(blocks == count)
            def _():
                together(k, count)

        @pl.when((k > 0) & (k < UNITS - 1))
        def _():
            hand_back(k - 1)

        return carry

    lax.fori_loop(-1, UNITS, step, 0)
    hand_back(UNITS - 1)

    for shift in range(1, NCP):
        other = peer(shift)
        send_pos(other).wait_send()
        for row in range(ROWS):
            send_piece(row, other).wait_send()
            send_out(row, other).wait_send()
            place = out.at[other * ROWS + row]
            pltpu.make_async_copy(place, place, out_recv.at[other * ROWS + row]).wait()
    for row in range(ROWS):
        own_out(row).wait()


def device_step(hidden, positions, *params):
    local_w, global_w = params[:11], params[11:]
    table = jnp.asarray(rope_lookup())
    hbm = pl.BlockSpec(memory_space=pltpu.HBM)
    vmem = pl.BlockSpec(memory_space=pltpu.VMEM)
    dma = pltpu.SemaphoreType.DMA
    return pl.pallas_call(
        kernel,
        out_shape=jax.ShapeDtypeStruct(hidden.shape, hidden.dtype),
        in_specs=[hbm, hbm, vmem] + [vmem] * 8 + [hbm] * 14,
        out_specs=pl.BlockSpec(memory_space=pl.ANY),
        scratch_shapes=[
            pltpu.VMEM((ROWS * NCP + 1, BLK, DIM), BF),
            pltpu.VMEM((NCP, NCP * ROWS, BLK), jnp.int32),
            pltpu.VMEM((2, DIM, QKV), BF),
            pltpu.VMEM((2, HEADS * HD, DIM), BF),
            pltpu.VMEM((2, DIM, 2 * FFN), BF),
            pltpu.VMEM((2, FFN, DIM), BF),
            pltpu.VMEM((2, 2, NCP * BLK, HD), BF),
            pltpu.VMEM((2, 2, NCP * BLK, HD), BF),
            pltpu.VMEM((HEADS, BLK, HD), BF),
            pltpu.VMEM((2, BLK, HEADS * HD), BF),
            pltpu.VMEM((HEADS, BLK, NCP * BLK), F32),
            pltpu.VMEM((BLK, FFN), BF),
            pltpu.VMEM((BLK, DIM), BF),
            pltpu.VMEM((BLK, DIM), BF),
            pltpu.VMEM((BLK, DIM), BF),
            pltpu.VMEM((BLK, DIM), BF),
            pltpu.VMEM((BLK, DIM), BF),
            pltpu.VMEM((4, BLK, HALF), F32),
            pltpu.VMEM((4, BLK, HALF), F32),
            pltpu.VMEM((4, BLK, 128), F32),
            pltpu.VMEM((8, 8, DIM), F32),
            dma((2, 7)),
            dma((ROWS, NCP)),
            dma((ROWS * NCP,)),
            dma((NCP,)),
            dma((NCP,)),
            dma((ROWS, NCP)),
            dma((NCP * ROWS,)),
        ],
        compiler_params=pltpu.CompilerParams(
            collective_id=0, has_side_effects=True, vmem_limit_bytes=67043328
        ),
        name="layers",
    )(hidden, positions, table, *local_w[7:], *global_w[7:], *local_w[:7], *global_w[:7])


def solution(mesh):
    specs_in = tuple([P("dp", "cp"), P("dp", "cp")] + [P()] * 22)
    return jax.shard_map(device_step, mesh=mesh, in_specs=specs_in, out_specs=P("dp", "cp"), check_vma=False)
```

```python
import functools

import jax
import jax.numpy as jnp
import numpy as np
from jax import lax
from jax.experimental import pallas as pl
from jax.experimental.pallas import tpu as pltpu
from jax.sharding import PartitionSpec as P

DIM = 640
HEADS = 4
HD = 256
HALF = HD // 2
FFN = 2048
WINDOW = 512
EPSILON = 1e-6
THETA = 10000.0
SOFT_CAP = 50.0
LOG2E = 1.4426950408889634
BLK = 256
NCP = 4
ROWS = 4
UNITS = ROWS * NCP * 2
QKV = HEADS * HD + 2 * HD
FCH = 512
NROW = 64
NCH = {0: 256, 256: 256, 512: 128}
LOW = 64
HIGH = 32
BF = jnp.bfloat16
F32 = jnp.float32
MESH = pl.DeviceIdType.MESH


def rope_lookup():
    inv_freq = THETA ** (-(np.arange(HALF, dtype=np.float64) * 2.0 / HD))
    table = np.zeros((128, 4 * HALF), np.float64)
    high = np.arange(HIGH)[:, None] * float(LOW) * inv_freq
    low = np.arange(LOW)[:, None] * inv_freq
    table[:HIGH, 0:HALF] = np.cos(high)
    table[:HIGH, HALF : 2 * HALF] = np.sin(high)
    table[HIGH : HIGH + LOW, 2 * HALF : 3 * HALF] = np.cos(low)
    table[HIGH : HIGH + LOW, 3 * HALF :] = np.sin(low)
    parts = []
    rest = table
    for _ in range(3):
        part = rest.astype(jnp.bfloat16)
        parts.append(part)
        rest = rest - part.astype(np.float64)
    return np.concatenate(parts, axis=0)


def dot(lhs, rhs):
    return jnp.dot(lhs, rhs, preferred_element_type=F32)


def rms(wide, gain):
    mean_sq = jnp.mean(wide * wide, axis=-1, keepdims=True)
    tall = (wide * lax.rsqrt(mean_sq + EPSILON)).reshape(-1, 8, DIM) * gain[None]
    return tall.reshape(-1, DIM).astype(BF)


def unit(k):
    stream = lax.rem(k, 2)
    turn = k // 2
    layer = lax.rem(turn, 2)
    piece = lax.rem(turn // 2, NCP)
    row = (turn // (2 * NCP)) * 2 + stream
    return stream, layer, piece, row


def kernel(hid, pos, table, *rest):
    scales = rest[:8]
    weights = rest[8:22]
    out = rest[22]
    (x_buf, pos_buf, w_qkv, w_o, w_gu, w_d, k_buf, v_buf, q_buf, o_buf, e_buf, h_buf, a_buf, m_buf, t_buf, d_buf, mid_buf, cos_buf,
     sin_buf, qp_buf, gains, w_sem, in_send, in_recv, pos_send, pos_recv, out_send, out_recv) = rest[23:]
    me = lax.axis_index("cp")

    def weight_copies(layer):
        w_q, w_k, w_v, wo, wg, wu, wd = weights[7 * layer : 7 * layer + 7]
        places = (
            (w_q, w_qkv.at[layer, :, 0:1024]),
            (w_k, w_qkv.at[layer, :, 1024:1280]),
            (w_v, w_qkv.at[layer, :, 1280:1536]),
            (wo, w_o.at[layer]),
            (wg, w_gu.at[layer, :, 0:FFN]),
            (wu, w_gu.at[layer, :, FFN : 2 * FFN]),
            (wd, w_d.at[layer]),
        )
        return [pltpu.make_async_copy(src, dst, w_sem.at[layer, i]) for i, (src, dst) in enumerate(places)]

    def peer(shift):
        return lax.rem(me + shift, NCP)

    def send_piece(row, dest):
        return pltpu.make_async_remote_copy(
            src_ref=hid.at[dest * ROWS + row],
            dst_ref=x_buf.at[row * NCP + me],
            send_sem=in_send.at[row, dest],
            recv_sem=in_recv.at[row * NCP + me],
            device_id={"cp": dest},
            device_id_type=MESH,
        )

    def own_piece(row):
        return pltpu.make_async_copy(hid.at[me * ROWS + row], x_buf.at[row * NCP + me], in_recv.at[row * NCP + me])

    def send_pos(dest):
        return pltpu.make_async_remote_copy(
            src_ref=pos,
            dst_ref=pos_buf.at[me],
            send_sem=pos_send.at[dest],
            recv_sem=pos_recv.at[me],
            device_id={"cp": dest},
            device_id_type=MESH,
        )

    def own_pos():
        return pltpu.make_async_copy(pos, pos_buf.at[me], pos_recv.at[me])

    def send_out(row, piece):
        return pltpu.make_async_remote_copy(
            src_ref=x_buf.at[row * NCP + piece],
            dst_ref=out.at[me * ROWS + row],
            send_sem=out_send.at[row, piece],
            recv_sem=out_recv.at[me * ROWS + row],
            device_id={"cp": piece},
            device_id_type=MESH,
        )

    def own_out(row):
        return pltpu.make_async_copy(x_buf.at[row * NCP + me], out.at[me * ROWS + row], out_send.at[row, me])

    for copy in weight_copies(0)[:3]:
        copy.start()
    own_piece(0).start()
    own_pos().start()
    own_piece(1).start()

    barrier = pltpu.get_barrier_semaphore()
    for shift in range(1, NCP):
        pl.semaphore_signal(barrier, inc=1, device_id={"cp": peer(shift)}, device_id_type=MESH)
    pl.semaphore_wait(barrier, NCP - 1)

    core = lax.rem(me, 2)
    partner = me + 1 - 2 * core
    far_0 = lax.rem(me + 2 - core, NCP)
    far_1 = lax.rem(me + 3 - core, NCP)
    for shift in range(1, NCP):
        send_pos(peer(shift)).start()
    for row in range(2):
        send_piece(row, partner).start()

    @pl.when(core == 0)
    def _():
        for row in range(2):
            send_piece(row, far_0).start()
            send_piece(row, far_1).start()

    for copy in weight_copies(0)[3:] + weight_copies(1):
        copy.start()
    for row in range(2, ROWS):
        own_piece(row).start()
    for i in range(8):
        gains[i] = jnp.broadcast_to(1.0 + scales[i][...].reshape(1, DIM), (8, DIM))
    own_pos().wait()
    for shift in range(1, NCP):
        src = peer(shift)
        pltpu.make_async_copy(pos_buf.at[src], pos_buf.at[src], pos_recv.at[src]).wait()

    def positions_of(piece, row):
        return pos_buf[piece, pl.ds(me * ROWS + row, 1), :].astype(F32)

    def receive(k):
        _, _, piece, row = unit(k)
        x_ref = x_buf.at[row * NCP + piece]
        pltpu.make_async_copy(x_ref, x_ref, in_recv.at[row * NCP + piece]).wait()

    def rope(stream, index, half):
        piece = lax.rem(index, NCP)
        row = jnp.minimum(index // NCP, 1) * 2 + stream
        slot = stream * 2 + lax.rem(index, 2)
        spot = pl.multiple_of(half * 128, 128)
        whole_row = positions_of(piece, row)
        row_pos = jnp.where(half == 0, whole_row[:, :128], whole_row[:, 128:])
        col_pos = jnp.transpose(jnp.broadcast_to(row_pos, (128, 128)))
        whole = col_pos.astype(jnp.int32)
        lane = lax.broadcasted_iota(jnp.int32, (128, 128), 1)
        hit = jnp.where((lane == (whole >> 6)) | (lane == (whole & (LOW - 1)) + HIGH), 1.0, 0.0).astype(BF)
        found = dot(jnp.concatenate([hit, hit], axis=1), table[0:256, :]) + dot(hit, table[256:384, :])
        c_hi, s_hi = found[:, 0:HALF], found[:, HALF : 2 * HALF]
        c_lo, s_lo = found[:, 2 * HALF : 3 * HALF], found[:, 3 * HALF :]
        qp_buf[slot, pl.ds(spot, 128), :] = col_pos
        cos_buf[slot, pl.ds(spot, 128), :] = c_hi * c_lo - s_hi * s_lo
        sin_buf[slot, pl.ds(spot, 128), :] = s_hi * c_lo + c_hi * s_lo

    def enter(k):
        _, layer, piece, row = unit(k)
        for lo in range(0, BLK, NROW):
            part = x_buf[row * NCP + piece, lo : lo + NROW, :].astype(F32)
            a_buf[lo : lo + NROW, :] = rms(part, gains[layer * 4])

    def attend(k, count):
        stream, layer, piece, row = unit(k)
        turn = stream * 2 + lax.rem(piece, 2)
        cos_t, sin_t = cos_buf[turn], sin_buf[turn]
        spot = pl.multiple_of(piece * BLK, BLK)
        keys = count * BLK
        first = piece - (count - 1)
        base = pl.multiple_of(first * BLK, BLK)
        below = lax.broadcasted_iota(jnp.int32, (128, 128), 0) >= lax.broadcasted_iota(jnp.int32, (128, 128), 1)
        window = jnp.where(layer == 0, float(WINDOW), 65536.0)
        q_low = qp_buf[turn] - window
        totals = {}

        def rotate(raw):
            wide = raw.astype(BF).astype(F32)
            one, two = wide[:, :HALF], wide[:, HALF:]
            return one * cos_t - two * sin_t, two * cos_t + one * sin_t

        def key_value():
            normed = a_buf[...]
            one, two = rotate(dot(normed, w_qkv[layer, :, 1024:1280]))
            k_buf[stream, layer, pl.ds(spot, BLK), :HALF] = one.astype(BF)
            k_buf[stream, layer, pl.ds(spot, BLK), HALF:] = two.astype(BF)
            v_buf[stream, layer, pl.ds(spot, BLK), :] = dot(normed, w_qkv[layer, :, 1280:1536]).astype(BF)

        def query(head):
            one, two = rotate(dot(a_buf[...], w_qkv[layer, :, head * HD : (head + 1) * HD]))
            q_buf[head, :, :HALF] = (one * HD**-0.5).astype(BF)
            q_buf[head, :, HALF:] = (two * HD**-0.5).astype(BF)

        def weigh(raw):
            return jnp.exp2(jnp.tanh(raw * (1.0 / SOFT_CAP)) * (SOFT_CAP * LOG2E))

        def score(head, j):
            key = k_buf[stream, layer, pl.ds(base + j * BLK, BLK), :]
            raw = lax.dot_general(q_buf[head], key, (((1,), (1,)), ((), ())), preferred_element_type=F32)
            if j == count - 1:
                early = jnp.where(below, weigh(raw[:128, :128]), 0.0)
                late = weigh(raw[128:, :128])
                rest = jnp.where(below, weigh(raw[128:, 128:]), 0.0)
                e_buf[head, :128, j * BLK : j * BLK + 128] = early
                e_buf[head, 128:, j * BLK : j * BLK + 128] = late
                e_buf[head, :128, j * BLK + 128 : (j + 1) * BLK] = jnp.zeros((128, 128), F32)
                e_buf[head, 128:, j * BLK + 128 : (j + 1) * BLK] = rest
                part = jnp.concatenate([early, late + rest], axis=0)
            else:
                soft = weigh(raw)
                if count < NCP:
                    k_pos = positions_of(first + j, row)
                    halves = []
                    for lo in (0, 128):
                        halves.append(jnp.where(q_low < k_pos[:, lo : lo + 128], soft[:, lo : lo + 128], 0.0))
                    soft = jnp.concatenate(halves, axis=1)
                e_buf[head, :, j * BLK : (j + 1) * BLK] = soft
                part = soft[:, :128] + soft[:, 128:]
            totals[head] = part if j == 0 else totals[head] + part
            if j == count - 1:
                totals[head] = 1.0 / jnp.sum(totals[head], axis=-1, keepdims=True)

        def mix(head):
            prob = (e_buf[head, :, 0:keys] * totals[head]).astype(BF)
            mixed = dot(prob, v_buf[stream, layer, pl.ds(base, keys), :])
            o_buf[stream, :, head * HD : (head + 1) * HD] = mixed.astype(BF)

        return key_value, query, score, mix

    def finish(k):
        stream, layer, piece, row = unit(k)
        kept = {}

        def project(lo):
            t_buf[:, lo : lo + NCH[lo]] = dot(o_buf[stream], w_o[layer, :, lo : lo + NCH[lo]]).astype(BF)

        def norms():
            for lo in range(0, BLK, NROW):
                delta = rms(t_buf[lo : lo + NROW, :].astype(F32), gains[layer * 4 + 1])
                part = x_buf[row * NCP + piece, lo : lo + NROW, :].astype(F32)
                mid = (part + delta.astype(F32)).astype(BF)
                mid_buf[lo : lo + NROW, :] = mid
                m_buf[lo : lo + NROW, :] = rms(mid.astype(F32), gains[layer * 4 + 2])

        def mlp(lo):
            normed_mid = m_buf[...]
            gate = dot(normed_mid, w_gu[layer, :, lo : lo + FCH]).astype(BF).astype(F32)
            up = dot(normed_mid, w_gu[layer, :, FFN + lo : FFN + lo + FCH]).astype(BF).astype(F32)
            inner = gate * (0.7978845608028654 + (0.7978845608028654 * 0.044715) * (gate * gate))
            h_buf[:, lo : lo + FCH] = ((0.5 * gate) * (1.0 + jnp.tanh(inner)) * up).astype(BF)

        def down(lo):
            d_buf[:, lo : lo + NCH[lo]] = dot(h_buf[...], w_d[layer, :, lo : lo + NCH[lo]]).astype(BF)

        return project, norms, mlp, down

    def last(k):
        _, layer, piece, row = unit(jnp.maximum(k, 0))
        slot = jnp.where(k < 0, ROWS * NCP, row * NCP + piece)
        for lo in range(0, BLK, NROW):
            delta = rms(d_buf[lo : lo + NROW, :].astype(F32), gains[layer * 4 + 3])
            part = mid_buf[lo : lo + NROW, :].astype(F32)
            x_buf[slot, lo : lo + NROW, :] = (part + delta.astype(F32)).astype(BF)

    def attend_alone(k, count):
        key_value, query, score, mix = attend(k, count)
        key_value()
        for head in range(HEADS):
            query(head)
        for head in range(HEADS):
            for j in range(count):
                score(head, j)
        for head in range(HEADS):
            mix(head)

    def finish_alone(k):
        project, norms, mlp, down = finish(k)
        for lo in NCH:
            project(lo)
        norms()
        for lo in range(0, FFN, FCH):
            mlp(lo)
        for lo in NCH:
            down(lo)

    def together(k, count):
        key_value, query, score, mix = attend(k + 1, count)
        project, norms, mlp, down = finish(k)
        stream, layer, _, _ = unit(k + 1)
        for lo in NCH:
            project(lo)
        last(k - 1)
        enter(k + 1)
        rope(stream, (k + 1) // 4 + 1, layer)
        norms()
        key_value()
        for head in range(HEADS):
            query(head)
        softmax = []
        for head in range(HEADS):
            softmax += [functools.partial(score, head, j) for j in range(count)]
            if head > 0:
                softmax.append(functools.partial(mix, head - 1))
        softmax.append(functools.partial(mix, HEADS - 1))
        dense = [functools.partial(mlp, lo) for lo in range(0, FFN, FCH)] + [functools.partial(down, lo) for lo in NCH]
        order = [((i + 0.5) / len(softmax), f) for i, f in enumerate(softmax)]
        order += [((i + 0.5) / len(dense), f) for i, f in enumerate(dense)]
        for _, stage in sorted(order, key=lambda pair: pair[0]):
            stage()

    def hand_back(k):
        _, layer, piece, row = unit(k)

        @pl.when((layer == 1) & (piece == me))
        def _():
            own_out(row).start()

        @pl.when((layer == 1) & (piece != me))
        def _():
            send_out(row, piece).start()

    d_buf[...] = jnp.zeros((BLK, DIM), BF)
    mid_buf[...] = jnp.zeros((BLK, DIM), BF)
    for stream in range(2):
        for half in range(2):
            rope(stream, 0, half)
    for copy in weight_copies(0)[:3]:
        copy.wait()

    def step(k, carry):
        after = k + 1
        stream, layer, piece, row = unit(after)
        alone = (k == 0) & (me >= 2)
        early = (k == UNITS - 2) & (me < 2)
        opening = k < 0
        closing = k == UNITS - 1

        @pl.when(k == 0)
        def _():
            for copy in weight_copies(0)[3:]:
                copy.wait()

        @pl.when((k == 1) & (core == 1))
        def _():
            for r in range(2):
                send_piece(r, far_0).start()
                send_piece(r, far_1).start()

        @pl.when((piece == 1) & (layer == 0) & (row < ROWS - 2))
        def _():
            for dest in (partner, far_0, far_1):
                send_piece(row + 2, dest).start()

        @pl.when(k == 1)
        def _():
            for copy in weight_copies(1):
                copy.wait()

        @pl.when(alone | early | closing)
        def _():
            @pl.when(alone | early | (me >= 2))
            def _():
                last(k - 1)

            @pl.when(closing & (me >= 2))
            def _():
                hand_back(k - 1)

            finish_alone(k)
            last(k)

            @pl.when(early)
            def _():
                hand_back(k)

        @pl.when((layer == 0) & (k < UNITS - 1))
        def _():
            receive(after)

        @pl.when(alone | opening)
        def _():
            enter(after)
            attend_alone(after, 1)
            rope(stream, after // 4 + 1, layer)

        @pl.when(early)
        def _():
            enter(after)
            attend_alone(after, NCP)

        blocks = jnp.where(layer == 0, jnp.minimum(piece, 2), piece) + 1
        blocks = jnp.where(alone | early | opening | closing, 0, blocks)
        for count in range(1, NCP + 1):
            @pl.when(blocks == count)
            def _():
                together(k, count)

        @pl.when((k > 0) & (k < UNITS - 1))
        def _():
            hand_back(k - 1)

        return carry

    lax.fori_loop(-1, UNITS, step, 0)
    hand_back(UNITS - 1)

    for shift in range(1, NCP):
        other = peer(shift)
        send_pos(other).wait_send()
        for row in range(ROWS):
            send_piece(row, other).wait_send()
            send_out(row, other).wait_send()
            place = out.at[other * ROWS + row]
            pltpu.make_async_copy(place, place, out_recv.at[other * ROWS + row]).wait()
    for row in range(ROWS):
        own_out(row).wait()


def device_step(hidden, positions, *params):
    local_w, global_w = params[:11], params[11:]
    table = jnp.asarray(rope_lookup())
    hbm = pl.BlockSpec(memory_space=pltpu.HBM)
    vmem = pl.BlockSpec(memory_space=pltpu.VMEM)
    dma = pltpu.SemaphoreType.DMA
    return pl.pallas_call(
        kernel,
        out_shape=jax.ShapeDtypeStruct(hidden.shape, hidden.dtype),
        in_specs=[hbm, hbm, vmem] + [vmem] * 8 + [hbm] * 14,
        out_specs=pl.BlockSpec(memory_space=pl.ANY),
        scratch_shapes=[
            pltpu.VMEM((ROWS * NCP + 1, BLK, DIM), BF),
            pltpu.VMEM((NCP, NCP * ROWS, BLK), jnp.int32),
            pltpu.VMEM((2, DIM, QKV), BF),
            pltpu.VMEM((2, HEADS * HD, DIM), BF),
            pltpu.VMEM((2, DIM, 2 * FFN), BF),
            pltpu.VMEM((2, FFN, DIM), BF),
            pltpu.VMEM((2, 2, NCP * BLK, HD), BF),
            pltpu.VMEM((2, 2, NCP * BLK, HD), BF),
            pltpu.VMEM((HEADS, BLK, HD), BF),
            pltpu.VMEM((2, BLK, HEADS * HD), BF),
            pltpu.VMEM((HEADS, BLK, NCP * BLK), F32),
            pltpu.VMEM((BLK, FFN), BF),
            pltpu.VMEM((BLK, DIM), BF),
            pltpu.VMEM((BLK, DIM), BF),
            pltpu.VMEM((BLK, DIM), BF),
            pltpu.VMEM((BLK, DIM), BF),
            pltpu.VMEM((BLK, DIM), BF),
            pltpu.VMEM((4, BLK, HALF), F32),
            pltpu.VMEM((4, BLK, HALF), F32),
            pltpu.VMEM((4, BLK, 128), F32),
            pltpu.VMEM((8, 8, DIM), F32),
            dma((2, 7)),
            dma((ROWS, NCP)),
            dma((ROWS * NCP,)),
            dma((NCP,)),
            dma((NCP,)),
            dma((ROWS, NCP)),
            dma((NCP * ROWS,)),
        ],
        compiler_params=pltpu.CompilerParams(
            collective_id=0, has_side_effects=True, vmem_limit_bytes=67043328
        ),
        name="layers",
    )(hidden, positions, table, *local_w[7:], *global_w[7:], *local_w[:7], *global_w[:7])


def solution(mesh):
    specs_in = tuple([P("dp", "cp"), P("dp", "cp")] + [P()] * 22)
    return jax.shard_map(device_step, mesh=mesh, in_specs=specs_in, out_specs=P("dp", "cp"), check_vma=False)
```
